32 devices in a mesh: mem: 8 (over y, x, core), col: 4 (over z).
Axes of the slice: x: 2, y: 2, z: 4, core: 2. Of those that a mesh axis runs over, the one named last changes fastest.
Arguments:
- background_trials: bfloat16 [256, 4, 32, 512], P('mem', None, None, 'col'), may hold values from -6 to 6
- region_active_tally: int32 [8, 16], P('mem', 'col'), may hold values from 256 to 2048, as said below
- sensed_component: int32 [8, 16, 2048], P('mem', 'col'), may hold values from 0 to 1919
- distance_bucket: int32 [8, 16, 2048], P('mem', 'col'), may hold values from 0 to 15
- sensor_readings: float32 [8, 16, 2048], P('mem', 'col'), may hold values from -6 to 6
- inverse_noise_variance: float32 [8, 16, 2048], P('mem', 'col'), may hold values from 0.25 to 4
- localization_factors: float32 [16], replicated, may hold values from 0.05 to 1
Outputs:
- analysis: bfloat16 [256, 4, 32, 512], P('mem', None, None, 'col')
The draws below stay inside these ranges and needn't reach their ends.
Inputs may be any that keep to these rules, and one draw needn't show every extreme that they name: `region_active_tally`: observations of a patch fill its first slots; some patch has exactly 2048 live observations. `sensed_component`: window entry in the order given in the reference program.
All inputs are finite; a program needn't handle non-finite values.
Results may differ from the reference program's by a relative error of at most 0.0063.
Values may be sent and summed in bfloat16 or wider, within the bound.
No kernel may reach another device: no remote copies, remote signals or barrier semaphores. Data moves between devices by JAX's collectives and lax.ppermute only.
A program may use at most 64 MiB of HBM per device.

```python
import math
import jax
import jax.numpy as jnp
from jax import lax

NUMBER_OF_RUNS = 256
VERTICAL_UNKNOWNS = 4
STRIP_DEPTH = 4
SECTOR_SPAN = 32
REACH_MARGIN = 4
OBS = 2048
CLASSES = 16
ITERS = 4
LATITUDE_LINES = 32
LONGITUDE_LINES = 512
NPY = 8
NPX = 16


def draw_region_active_tally(key, part):
    first_key, second_key, third_key = jax.random.split(jax.random.fold_in(key, 11), 3)
    base_count = jax.random.randint(first_key, (NPY * NPX,), OBS // 8, OBS // 2 + 1)
    is_busy = jax.random.randint(second_key, (NPY * NPX,), 0, 8) == 0
    full_spot = jax.random.randint(third_key, (), 0, NPY * NPX)
    is_full = jnp.logical_or(is_busy, jnp.arange(NPY * NPX, dtype=jnp.int32) == full_spot)
    counts_all = jnp.where(is_full, OBS, base_count)
    return counts_all.reshape(NPY, NPX).astype(jnp.int32)


def touch_ends(values, rng, least, high):
    longest = values.shape.index(max(values.shape))
    spots = []
    for shift in (0, 1):
        where = [jax.random.randint(jax.random.fold_in(rng, axis), (), 0, length) for axis, length in enumerate(values.shape)]
        where[longest] = (where[longest] + shift) % values.shape[longest]
        spots.append(tuple(where))
    return values.at[spots[0]].set(least).at[spots[1]].set(high)


def block_scale(stream_key, dims, cuts, least, largest):
    gain = 1.0
    for position, blocks in cuts:
        heights = jax.random.uniform(jax.random.fold_in(jax.random.fold_in(stream_key, 6), position), (blocks,), jnp.float32, least / len(cuts), largest / len(cuts))
        gain = gain * jnp.repeat(jnp.exp(heights), dims[position] // blocks).reshape((-1,) + (1,) * (len(dims) - 1 - position))
    return gain


def centred(key, shape, spread, bound, cuts=(), held_as=jnp.bfloat16):
    array = spread * jax.random.normal(key, shape, jnp.float32)
    if cuts:
        array = array * block_scale(key, shape, cuts, -0.22, 0.18)
    return jnp.clip(array, -bound, bound).astype(held_as)


def setup_inputs(seed: int = 0) -> dict:
    streams_of = jax.random.split(jax.random.key(seed), 8)
    background_trials = centred(streams_of[0], (NUMBER_OF_RUNS, VERTICAL_UNKNOWNS, LATITUDE_LINES, LONGITUDE_LINES), 1.0, 6.0, ((0, 8), (3, 4)))
    region_active_tally = draw_region_active_tally(jax.random.fold_in(streams_of[7], 71), 0)
    sensed_component = touch_ends(jax.random.randint(streams_of[2], (NPY, NPX, OBS), 0, VERTICAL_UNKNOWNS * (STRIP_DEPTH + 2 * REACH_MARGIN) * (SECTOR_SPAN + 2 * REACH_MARGIN)), jax.random.fold_in(streams_of[2], 1), 0, (VERTICAL_UNKNOWNS * (STRIP_DEPTH + 2 * REACH_MARGIN) * (SECTOR_SPAN + 2 * REACH_MARGIN)) - 1).astype(jnp.int32)
    distance_bucket = touch_ends(jax.random.randint(streams_of[3], (NPY, NPX, OBS), 0, CLASSES), jax.random.fold_in(streams_of[3], 1), 0, CLASSES - 1).astype(jnp.int32)
    sensor_readings = centred(streams_of[4], (NPY, NPX, OBS), 1.0, 6.0, ((0, 8), (1, 4)), jnp.float32)
    inverse_noise_variance = jnp.clip(jnp.exp(math.log(4.0) - 2.7725887 * jax.random.uniform(streams_of[5], (NPY, NPX, OBS), jnp.float32) ** block_scale(streams_of[5], (NPY, NPX, OBS), ((0, 8), (1, 4)), -0.2, 0.2)), 0.25, 4.0)
    localization_factors = jnp.clip(jnp.exp(jax.random.uniform(streams_of[6], (CLASSES,), jnp.float32, math.log(0.05), math.log(1.0))), 0.05, 1.0)
    return {"background_trials": background_trials, "region_active_tally": region_active_tally, "sensed_component": sensed_component, "distance_bucket": distance_bucket, "sensor_readings": sensor_readings, "inverse_noise_variance": inverse_noise_variance, "localization_factors": localization_factors}


inflation = 1.1

def lookup(class_ids, weight_table):
    table_slots = jnp.arange(weight_table.shape[0], dtype=jnp.int32)
    return lax.optimization_barrier(jnp.sum(jnp.where(class_ids[..., None] == table_slots, weight_table, 0.0), axis=-1))

def analyse_patch(viewing_frame, window_average, live_count, cell_ids, class_ids, values, inv_var, weight_table):
    trial_flattened = viewing_frame.shape[0]
    physical_quantity_stack = viewing_frame.shape[1]
    deviation_matrix = (viewing_frame.astype(jnp.float32) - window_average).astype(jnp.bfloat16)
    flattened = deviation_matrix.reshape(trial_flattened, -1)
    observed = jnp.take(flattened, cell_ids, axis=1)
    innovation = values - jnp.take(window_average.reshape(-1), cell_ids)
    is_live = jnp.arange(cell_ids.shape[0], dtype=jnp.int32) < live_count
    weight = jnp.where(is_live, inv_var * lookup(class_ids, weight_table), 0.0)
    scaled = (observed.astype(jnp.float32) * weight).astype(jnp.bfloat16)
    gram_sum = jnp.dot(scaled, observed.T, preferred_element_type=jnp.float32)
    forcing = jnp.dot(scaled.astype(jnp.float32), innovation, precision=lax.Precision.HIGHEST)
    identity = jnp.eye(trial_flattened, dtype=jnp.float32)
    gram_sum = gram_sum + (trial_flattened - 1) / inflation * identity
    norm_scale = jnp.sqrt(jnp.sum(gram_sum * gram_sum))
    iterate = gram_sum / norm_scale
    inverse_root = identity
    for sweep_id in range(ITERS):
        factor = 1.5 * identity - 0.5 * jnp.dot(inverse_root, iterate, precision=lax.Precision.HIGHEST)
        iterate = jnp.dot(iterate, factor, precision=lax.Precision.HIGHEST)
        inverse_root = jnp.dot(factor, inverse_root, precision=lax.Precision.HIGHEST)
    partial_shift = jnp.dot(inverse_root, forcing, precision=lax.Precision.HIGHEST)
    mean_shift = jnp.dot(inverse_root, partial_shift, precision=lax.Precision.HIGHEST) / norm_scale
    transform = jnp.sqrt((trial_flattened - 1.0) / norm_scale) * inverse_root + mean_shift[:, None]
    transform = transform.astype(jnp.bfloat16)
    own_anomaly = deviation_matrix[:, :, REACH_MARGIN:REACH_MARGIN + STRIP_DEPTH, REACH_MARGIN:REACH_MARGIN + SECTOR_SPAN].reshape(trial_flattened, -1)
    inner_midpoint = window_average[:, REACH_MARGIN:REACH_MARGIN + STRIP_DEPTH, REACH_MARGIN:REACH_MARGIN + SECTOR_SPAN].reshape(-1)
    result = jnp.dot(transform.T, own_anomaly, preferred_element_type=jnp.float32) + inner_midpoint
    return result.astype(jnp.bfloat16).reshape(trial_flattened, physical_quantity_stack, STRIP_DEPTH, SECTOR_SPAN)

def reference(background_trials, region_active_tally, sensed_component, distance_bucket, sensor_readings, inverse_noise_variance, localization_factors):
    trial_flattened, physical_quantity_stack, latitude_sum, longitude_sum = background_trials.shape
    predicted_average = lax.optimization_barrier(jnp.sum(background_trials, axis=0, dtype=jnp.float32)) / trial_flattened
    margined_predictions = jnp.pad(background_trials, ((0, 0), (0, 0), (REACH_MARGIN, REACH_MARGIN), (REACH_MARGIN, REACH_MARGIN)))
    enlarged_midpoint = jnp.pad(predicted_average, ((0, 0), (REACH_MARGIN, REACH_MARGIN), (REACH_MARGIN, REACH_MARGIN)))
    patch_cols = longitude_sum // SECTOR_SPAN
    patch_total = latitude_sum // STRIP_DEPTH * patch_cols

    def one_patch(patch_index):
        row_id = patch_index // patch_cols
        col_id = patch_index % patch_cols
        topmost_offset = (row_id * STRIP_DEPTH).astype(jnp.int32)
        leftmost_offset = (col_id * SECTOR_SPAN).astype(jnp.int32)
        corner_point = jnp.zeros((), jnp.int32)
        viewing_frame = lax.dynamic_slice(margined_predictions, (corner_point, corner_point, topmost_offset, leftmost_offset), (trial_flattened, physical_quantity_stack, STRIP_DEPTH + 2 * REACH_MARGIN, SECTOR_SPAN + 2 * REACH_MARGIN))
        window_average = lax.dynamic_slice(enlarged_midpoint, (corner_point, topmost_offset, leftmost_offset), (physical_quantity_stack, STRIP_DEPTH + 2 * REACH_MARGIN, SECTOR_SPAN + 2 * REACH_MARGIN))
        return analyse_patch(viewing_frame, window_average, region_active_tally[row_id, col_id], sensed_component[row_id, col_id], distance_bucket[row_id, col_id], sensor_readings[row_id, col_id], inverse_noise_variance[row_id, col_id], localization_factors)
    blocks = lax.map(one_patch, jnp.arange(patch_total, dtype=jnp.int32))
    blocks = blocks.reshape(latitude_sum // STRIP_DEPTH, patch_cols, trial_flattened, physical_quantity_stack, STRIP_DEPTH, SECTOR_SPAN)
    return blocks.transpose(2, 3, 0, 4, 1, 5).reshape(trial_flattened, physical_quantity_stack, latitude_sum, longitude_sum)
```

```python
import functools
import jax
import jax.numpy as jnp
from jax import lax
from jax.experimental import pallas as pl
from jax.experimental.pallas import tpu as pltpu
from jax.sharding import PartitionSpec as P

DEPTH = 4
SPAN = 32
MARGIN = 4
ITERS = 4
LANES = 128
MAP_ROWS = 16
INFLATION = 1.1

f32 = jnp.float32
bf16 = jnp.bfloat16
i32 = jnp.int32
VMEM = pl.BlockSpec(memory_space=pltpu.VMEM)
SMEM = pl.BlockSpec(memory_space=pltpu.SMEM)
PARAMS = pltpu.CompilerParams(vmem_limit_bytes=24 * 1024 * 1024)


def iota(shape, dim):
    return lax.broadcasted_iota(i32, shape, dim)


def dot(a, b):
    return jnp.dot(a, b, preferred_element_type=f32)


def one_hot(condition):
    return jnp.where(condition, 1.0, 0.0).astype(bf16)


class Plan:
    def __init__(self, x_shape, count, states):
        self.members, self.states, self.rows, self.cols = x_shape
        self.count = count
        self.total = self.members * count
        self.patches = self.cols // SPAN
        self.bands = self.rows // DEPTH
        self.groups = self.bands // self.patches
        chips = count // 2
        if count % 2 == 0 and chips % self.patches == 0:
            self.place = [
                (2 * (i // 2 // self.patches) + i % 2, i // 2 % self.patches) for i in range(count)
            ]
        else:
            self.place = [(i // self.patches, i % self.patches) for i in range(count)]
        self.slot_bands = self.patches + min(2, self.groups - 1) if self.groups > 1 else self.patches
        self.full = self.slot_bands == self.patches + 2
        self.per_band = self.states + 1
        self.field = self.slot_bands * self.per_band
        self.map_groups = 4 * MAP_ROWS // self.members
        self.slot = self.field + self.map_groups
        self.index_of = {p: i for i, p in enumerate(self.place)}

    def first_band(self, group):
        low = self.patches * group - 1
        return low if self.full else max(low, 0)

    def band_slots(self, band):
        return [
            (g, band - self.first_band(g))
            for g in range(self.groups)
            if 0 <= band - self.first_band(g) < self.slot_bands
        ]


def side_source(lane, column, cols):
    eighth = lane % (2 * MARGIN)
    low = column * SPAN - MARGIN + eighth
    high = column * SPAN + SPAN + eighth - MARGIN
    return jnp.where(eighth < MARGIN, low, high)


def pack_kernel(plan, x_ref, buf_ref, up_ref, down_ref, turned, q_ref, side_ref):
    half = 16
    rows, cols = plan.rows, plan.cols
    span = half * rows
    r = iota((span, span), 0)
    k = iota((span, span), 1)
    perm = one_hot((r % half == k // rows) & (r // half == k % rows))
    for s in range(plan.states):
        for h in range(plan.members // half):
            piece = x_ref[h * half : (h + 1) * half, s].reshape(span, cols)
            turned[s, :, h * half : (h + 1) * half, :] = (
                dot(perm, piece).astype(bf16).reshape(rows, half, cols)
            )
    wide = DEPTH * cols
    r = iota((wide, wide), 0)
    k = iota((wide, wide), 1)
    q_ref[...] = one_hot(
        (r // cols == (k % LANES) // SPAN) & (r % cols == (k // LANES) * SPAN + k % SPAN)
    )
    n_side = (plan.patches + 2) * LANES
    col = iota((cols, n_side), 0)
    out = iota((cols, n_side), 1)
    column = out // LANES
    lane = out % LANES
    eighth = lane % (2 * MARGIN)
    source = side_source(lane, column, cols)
    to_up = (column == plan.patches) & (eighth < MARGIN)
    to_down = (column == plan.patches + 1) & (eighth >= MARGIN)
    source = jnp.where(column < plan.patches, source, -1)
    source = jnp.where(to_up, cols - MARGIN + eighth, source)
    source = jnp.where(to_down, eighth - MARGIN, source)
    hit = jnp.where(col == source, 1.0, 0.0)
    which = iota((1, n_side), 1) % LANES // (2 * MARGIN)
    for s in range(plan.states):
        for t in range(DEPTH):
            at = s * DEPTH + t
            side_ref[at * cols : (at + 1) * cols, :] = jnp.where(which == at, hit, 0.0).astype(bf16)
    lhs = [
        jnp.concatenate(
            [
                jnp.concatenate([turned[s, b * DEPTH + t] for b in range(plan.bands)], axis=0)
                for t in range(DEPTH)
            ],
            axis=1,
        )
        for s in range(plan.states)
    ]
    zero = jnp.zeros((plan.members, LANES), bf16)

    def put(band, inner, column, value):
        for g, position in plan.band_slots(band):
            buf_ref[plan.index_of[(g, column)], position * plan.per_band + inner] = value

    m = plan.members
    for s in range(plan.states):
        center = dot(lhs[s], q_ref[...]).astype(bf16)
        for b in range(plan.bands):
            for c in range(plan.patches):
                put(b, s, c, center[b * m : (b + 1) * m, c * LANES : (c + 1) * LANES])
    sides = dot(jnp.concatenate(lhs, axis=1), side_ref[...]).astype(bf16)
    for b in range(plan.bands):
        for c in range(plan.patches):
            put(b, plan.states, c, sides[b * m : (b + 1) * m, c * LANES : (c + 1) * LANES])
    at = plan.patches * LANES
    up_ref[...] = sides[:, at : at + LANES]
    down_ref[...] = sides[:, at + LANES : at + 2 * LANES]
    if plan.full:
        for c in range(plan.patches):
            for inner in range(plan.per_band):
                buf_ref[plan.index_of[(0, c)], inner] = zero
                last = (plan.slot_bands - 1) * plan.per_band + inner
                buf_ref[plan.index_of[(plan.groups - 1, c)], last] = zero


def split2(a):
    high = a.astype(bf16)
    return high, (a - high.astype(f32)).astype(bf16)


def window_place(entry):
    height = DEPTH + 2 * MARGIN
    width = SPAN + 2 * MARGIN
    plane = height * width
    state = sum((entry >= plane * n).astype(i32) for n in range(1, 4))
    rest = entry - state * plane
    row = (rest * 1639) >> 16
    col = rest - row * width
    band = row >> 2
    inner = row & 3
    center = (col >= MARGIN) & (col < MARGIN + SPAN)
    eighth = jnp.where(col < MARGIN, col, col - SPAN)
    lane = jnp.where(center, inner * SPAN + col - MARGIN, state * SPAN + inner * 2 * MARGIN + eighth)
    group = band * 5 + jnp.where(center, state, 4)
    return group, lane


def map_kernel(patches, table, count_ref, factor_ref, cell_ref, class_ref, value_ref, inv_ref, out_ref):
    slots = cell_ref.shape[1]
    group, lane = window_place(cell_ref[...])
    classes = class_ref[...]
    factor = jnp.zeros(classes.shape, f32)
    for n in range(table):
        factor = jnp.where(classes == n, factor_ref[n], factor)
    weight = inv_ref[...] * factor
    order = iota((1, slots), 1)
    for p in range(patches):
        live = jnp.where(order < count_ref[0, p], weight[p : p + 1], 0.0)
        hot = one_hot(iota((LANES, slots), 0) == lane[p : p + 1])
        pick = iota((MAP_ROWS, slots), 0) == group[p : p + 1]
        parts = []
        for source in (live, live * value_ref[p : p + 1]):
            for _ in range(3):
                high = source.astype(bf16).astype(f32)
                parts.append(jnp.where(pick, high, 0.0).astype(bf16))
                source = source - high
        maps = lax.dot_general(
            jnp.concatenate(parts, axis=0), hot, (((1,), (1,)), ((), ())), preferred_element_type=f32
        )
        n = MAP_ROWS
        w_high, w_low = split2(maps[:n] + maps[n : 2 * n] + maps[2 * n : 3 * n])
        v_high, v_low = split2(maps[3 * n : 4 * n] + maps[4 * n : 5 * n] + maps[5 * n :])
        out_ref[p] = jnp.concatenate([w_high, w_low, v_high, v_low], axis=0)


def join_kernel(plan, own_ref, buf_in, maps_ref, left_ref, right_ref, buf_ref):
    m = plan.members
    buf_ref[:, : plan.field] = buf_in[:, : plan.field]
    for b in range(plan.bands):
        for column, strip in ((0, left_ref), (plan.patches - 1, right_ref)):
            extra = strip[b * m : (b + 1) * m]
            for g, position in plan.band_slots(b):
                at = (plan.index_of[(g, column)], position * plan.per_band + plan.states)
                buf_ref[at] = buf_in[at] + extra
    for i, (g, c) in enumerate(plan.place):
        piece = jnp.where(own_ref[0] == g, maps_ref[c], jnp.zeros_like(maps_ref[c]))
        for n in range(plan.map_groups):
            buf_ref[i, plan.field + n] = piece[n * m : (n + 1) * m]


def mm3(ah, al, bh, bl):
    return dot(jnp.concatenate([ah, ah, al], axis=1), jnp.concatenate([bh, bl, bh], axis=0))


def analyse_kernel(plan, map_at, place_ref, x_ref, maps_ref, out_ref, xs, avgs, scaled, lead):
    total = plan.total
    sources, _, piece_rows, _ = x_ref.shape
    per_band, states, patches = plan.per_band, plan.states, plan.patches
    window = 3 * per_band * LANES
    group = place_ref[0]
    shift = place_ref[1]
    if not plan.full:
        blank = jnp.zeros((total, per_band * LANES), bf16)
        if plan.slot_bands == patches:
            edges = (0, patches + 1)
            for edge in edges:
                xs[:, edge * per_band * LANES : (edge + 1) * per_band * LANES] = blank
                avgs[edge * 8 : edge * 8 + 8] = jnp.zeros((8, LANES), f32)
        else:
            edge = jnp.where(shift == 1, 0, patches + 1)
            xs[:, pl.ds(pl.multiple_of(edge * per_band * LANES, LANES), per_band * LANES)] = blank
            avgs[pl.ds(pl.multiple_of(edge * 8, 8), 8)] = jnp.zeros((8, LANES), f32)
    for b in range(plan.slot_bands):
        means = []
        for inner in range(per_band):
            at = b * per_band + inner
            raw = jnp.concatenate([x_ref[n, at] for n in range(sources)], axis=0).astype(f32)
            mean = jnp.sum(raw, axis=0, keepdims=True) / total
            means.append(mean)
            lanes = pl.multiple_of((shift * per_band + at) * LANES, LANES)
            xs[:, pl.ds(lanes, LANES)] = (raw - mean).astype(bf16)
        means.append(jnp.zeros((8 - per_band, LANES), f32))
        avgs[pl.ds(pl.multiple_of((b + shift) * 8, 8), 8)] = jnp.concatenate(means, axis=0)
    eye = jnp.where(iota((total, total), 0) == iota((total, total), 1), 1.0, 0.0)
    grams, forcings, norms = [], [], []
    for q in range(patches):
        n_map = maps_ref.shape[1] - map_at
        maps = jnp.concatenate(
            [maps_ref[patches * group + q, map_at + n] for n in range(n_map)], axis=0
        ).astype(f32)
        n = MAP_ROWS
        weight = maps[:n] + maps[n : 2 * n]
        value = maps[2 * n : 3 * n] + maps[3 * n :]
        lead[...] = jnp.zeros_like(lead)
        for d in range(3):
            for inner in range(per_band):
                at = d * per_band + inner
                lanes = (q * per_band + at) * LANES
                w = weight[at : at + 1]
                here = slice(at * LANES, (at + 1) * LANES)
                scaled[q, :total, here] = (xs[:, lanes : lanes + LANES].astype(f32) * w).astype(bf16)
                row = (q + d) * 8 + inner
                v = value[at : at + 1] - w * avgs[row : row + 1]
                for part in range(3):
                    high = v.astype(bf16).astype(f32)
                    lead[part : part + 1, here] = high
                    v = v - high
        scaled[q, total:] = lead[...].astype(bf16)
        first = q * per_band * LANES
        both = lax.dot_general(
            scaled[q],
            xs[:, first : first + window],
            (((1,), (1,)), ((), ())),
            preferred_element_type=f32,
        )
        gram = both[:total] + ((total - 1) / INFLATION) * eye
        forcings.append(both[total : total + 1] + both[total + 1 : total + 2] + both[total + 2 : total + 3])
        norm = jnp.sqrt(jnp.sum(jnp.sum(gram * gram, axis=1, keepdims=True), axis=0, keepdims=True))
        norms.append(norm)
        grams.append(gram / norm)
    factors, iterates, roots = [], [], []
    for q in range(patches):
        y = split2(grams[q])
        f = split2(1.5 * eye - 0.5 * grams[q])
        iterates.append(split2(mm3(*y, *f)))
        roots.append(f)
    for sweep in range(1, ITERS):
        for q in range(patches):
            f = split2(1.5 * eye - 0.5 * mm3(*roots[q], *iterates[q]))
            if sweep + 1 < ITERS:
                iterates[q] = split2(mm3(*iterates[q], *f))
                roots[q] = split2(mm3(*roots[q], *f))
            else:
                roots[q] = mm3(*roots[q], *f)
    for q in range(patches):
        root = roots[q]
        force = jnp.broadcast_to(forcings[q], (8, total))
        part = jnp.dot(force, root, precision=lax.Precision.HIGHEST, preferred_element_type=f32)
        move = jnp.dot(part, root, precision=lax.Precision.HIGHEST, preferred_element_type=f32)
        move = move[:1] / norms[q]
        transform = (jnp.sqrt((total - 1.0) / norms[q]) * root + move).astype(bf16)
        first = (q + 1) * per_band * LANES
        analysed = dot(transform, xs[:, first : first + states * LANES])
        for s in range(states):
            row = (q + 1) * 8 + s
            value = (analysed[:, s * LANES : (s + 1) * LANES] + avgs[row : row + 1]).astype(bf16)
            for n in range(sources):
                out_ref[n, q * states + s] = value[n * piece_rows : (n + 1) * piece_rows]


def unpack_kernel(plan, in_ref, out_ref, q_ref, turned):
    half = 16
    m, rows, cols, states = plan.members, plan.rows, plan.cols, plan.states
    wide = DEPTH * cols
    r = iota((wide, wide), 0)
    k = iota((wide, wide), 1)
    q_ref[...] = one_hot(
        (k // cols == (r % LANES) // SPAN) & (k % cols == (r // LANES) * SPAN + r % SPAN)
    )
    for s in range(states):
        lhs = []
        for b in range(plan.bands):
            g, q = b // plan.patches, b % plan.patches
            lhs.append(
                jnp.concatenate(
                    [in_ref[plan.index_of[(g, c)], q * states + s] for c in range(plan.patches)], axis=1
                )
            )
        opened = dot(jnp.concatenate(lhs, axis=0), q_ref[...]).astype(bf16)
        for b in range(plan.bands):
            for t in range(DEPTH):
                turned[s, b * DEPTH + t] = opened[b * m : (b + 1) * m, t * cols : (t + 1) * cols]
    span = half * rows
    r = iota((span, span), 0)
    k = iota((span, span), 1)
    perm = one_hot((k % half == r // rows) & (k // half == r % rows))
    for s in range(states):
        for h in range(m // half):
            piece = turned[s, :, h * half : (h + 1) * half, :].reshape(span, cols)
            out_ref[h * half : (h + 1) * half, s] = (
                dot(perm, piece).astype(bf16).reshape(half, rows, cols)
            )


def shifts(axis):
    count = lax.axis_size(axis)
    forward = [(i, i + 1) for i in range(count - 1)]
    return forward, [(b, a) for a, b in forward]


def pack_plain(plan, x):
    m, s, b = plan.members, plan.states, plan.bands
    bands = x.reshape(m, s, b, DEPTH, plan.cols)
    center = bands.reshape(m, s, b, DEPTH, plan.patches, SPAN).transpose(4, 2, 1, 0, 3, 5)
    center = center.reshape(plan.patches, b, s, m, LANES)
    padded = jnp.pad(bands, ((0, 0),) * 4 + ((MARGIN, MARGIN),))
    sides = jnp.stack(
        [
            jnp.concatenate(
                [
                    padded[..., c * SPAN : c * SPAN + MARGIN],
                    padded[..., (c + 1) * SPAN + MARGIN : (c + 1) * SPAN + 2 * MARGIN],
                ],
                axis=-1,
            )
            for c in range(plan.patches)
        ]
    )
    sides = sides.transpose(0, 3, 1, 2, 4, 5).reshape(plan.patches, b, 1, m, LANES)
    whole = jnp.concatenate([center, sides], axis=2)
    whole = jnp.pad(whole, ((0, 0), (1, 1)) + ((0, 0),) * 3)
    slots = []
    for g, c in plan.place:
        first = plan.first_band(g) + 1
        piece = whole[c, first : first + plan.slot_bands].reshape(plan.field, m, LANES)
        slots.append(jnp.pad(piece, ((0, plan.map_groups), (0, 0), (0, 0))))
    empty = jnp.zeros_like(bands[..., :MARGIN])
    strips = []
    for pair in ((bands[..., -MARGIN:], empty), (empty, bands[..., :MARGIN])):
        strip = jnp.concatenate(pair, axis=-1).transpose(2, 0, 1, 3, 4)
        strips.append(strip.reshape(b * m, LANES))
    return jnp.stack(slots), strips[0], strips[1]


def unpack_plain(plan, arrived):
    m, s, b = plan.members, plan.states, plan.bands
    bands = []
    for band in range(b):
        g, q = band // plan.patches, band % plan.patches
        pieces = jnp.stack(
            [arrived[plan.index_of[(g, c)], q * s : (q + 1) * s] for c in range(plan.patches)]
        )
        pieces = pieces.reshape(plan.patches, s, m, DEPTH, SPAN).transpose(2, 1, 3, 0, 4)
        bands.append(pieces.reshape(m, s, DEPTH, plan.cols))
    return jnp.concatenate(bands, axis=2)


def local(x, tally, cells, classes, readings, inverse, factors):
    count = lax.axis_size("mem")
    plan = Plan(x.shape, count, x.shape[1])
    patches = plan.patches
    index = lax.axis_index("mem")
    aligned = plan.members % 16 == 0
    buffer = (count, plan.slot, plan.members, LANES)
    strip = (plan.bands * plan.members, LANES)
    if aligned:
        packed, upward, downward = pl.pallas_call(
            functools.partial(pack_kernel, plan),
            out_shape=(
                jax.ShapeDtypeStruct(buffer, bf16),
                jax.ShapeDtypeStruct(strip, bf16),
                jax.ShapeDtypeStruct(strip, bf16),
            ),
            in_specs=[VMEM],
            out_specs=(VMEM, VMEM, VMEM),
            scratch_shapes=[
                pltpu.VMEM((plan.states, plan.rows, plan.members, plan.cols), bf16),
                pltpu.VMEM((DEPTH * plan.cols, DEPTH * plan.cols), bf16),
                pltpu.VMEM((plan.states * DEPTH * plan.cols, (patches + 2) * LANES), bf16),
            ],
            compiler_params=PARAMS,
            name="pack",
        )(x)
    else:
        packed, upward, downward = pack_plain(plan, x)
    forward, backward = shifts("col")
    left = lax.ppermute(upward, "col", forward)
    right = lax.ppermute(downward, "col", backward)
    slots = cells.shape[-1]
    maps = pl.pallas_call(
        functools.partial(map_kernel, patches, factors.shape[0]),
        out_shape=jax.ShapeDtypeStruct((patches, 4 * MAP_ROWS, LANES), bf16),
        in_specs=[SMEM, SMEM, VMEM, VMEM, VMEM, VMEM],
        out_specs=VMEM,
        compiler_params=PARAMS,
        name="maps",
    )(
        tally,
        factors,
        cells.reshape(patches, slots),
        classes.reshape(patches, slots),
        readings.reshape(patches, slots),
        inverse.reshape(patches, slots),
    )
    if aligned:
        packed = pl.pallas_call(
            functools.partial(join_kernel, plan),
            out_shape=jax.ShapeDtypeStruct(buffer, bf16),
            in_specs=[SMEM, VMEM, VMEM, VMEM, VMEM],
            out_specs=VMEM,
            compiler_params=PARAMS,
            name="join",
        )((index // patches).reshape(1), packed, maps, left, right)
    else:
        for b in range(plan.bands):
            at = slice(b * plan.members, (b + 1) * plan.members)
            for column, extra in ((0, left[at]), (patches - 1, right[at])):
                for g, position in plan.band_slots(b):
                    here = position * plan.per_band + plan.states
                    packed = packed.at[plan.index_of[(g, column)], here].add(extra)
        for i, (g, c) in enumerate(plan.place):
            piece = jnp.where(index // patches == g, maps[c], 0).reshape(-1, plan.members, LANES)
            packed = packed.at[i, plan.field :].set(piece)
    arrived = lax.all_to_all(packed, "mem", split_axis=0, concat_axis=0, tiled=True)
    group = jnp.asarray([g for g, _ in plan.place], i32)[index]
    shift = jnp.where(group == 0, 0 if plan.full else 1, 0)
    where = jnp.stack([group, shift]).astype(i32)
    if aligned:
        fields, map_source, map_at = arrived, arrived, plan.field
        pieces = (count, plan.members)
    else:
        fields = arrived[:, : plan.field].transpose(1, 0, 2, 3).reshape(1, plan.field, plan.total, LANES)
        map_source = arrived[:, plan.field :].reshape(count, 1, 4 * MAP_ROWS, LANES)
        map_at = 0
        pieces = (1, plan.total)
    bands = (patches + 2) * plan.per_band
    analysed = pl.pallas_call(
        functools.partial(analyse_kernel, plan, map_at),
        out_shape=jax.ShapeDtypeStruct((pieces[0], patches * plan.states, pieces[1], LANES), bf16),
        in_specs=[SMEM, VMEM, VMEM],
        out_specs=VMEM,
        scratch_shapes=[
            pltpu.VMEM((plan.total, bands * LANES), bf16),
            pltpu.VMEM(((patches + 2) * 8, LANES), f32),
            pltpu.VMEM((patches, plan.total + 16, 3 * plan.per_band * LANES), bf16),
            pltpu.VMEM((16, 3 * plan.per_band * LANES), f32),
        ],
        compiler_params=PARAMS,
        name="analyse",
    )(where, fields, map_source)
    if not aligned:
        analysed = analysed.reshape(-1, count, plan.members, LANES).transpose(1, 0, 2, 3)
    returned = lax.all_to_all(analysed, "mem", split_axis=0, concat_axis=0, tiled=True)
    if not aligned:
        return unpack_plain(plan, returned)
    return pl.pallas_call(
        functools.partial(unpack_kernel, plan),
        out_shape=jax.ShapeDtypeStruct(x.shape, bf16),
        in_specs=[VMEM],
        out_specs=VMEM,
        scratch_shapes=[
            pltpu.VMEM((DEPTH * plan.cols, DEPTH * plan.cols), bf16),
            pltpu.VMEM((plan.states, plan.rows, plan.members, plan.cols), bf16),
        ],
        compiler_params=PARAMS,
        name="unpack",
    )(returned)


def solution(mesh):
    placed = (
        P("mem", None, None, "col"),
        P("mem", "col"),
        P("mem", "col", None),
        P("mem", "col", None),
        P("mem", "col", None),
        P("mem", "col", None),
        P(),
    )
    return jax.shard_map(
        local, mesh=mesh, in_specs=placed, out_specs=P("mem", None, None, "col"), check_vma=False
    )
```

```python
import functools
import jax
import jax.numpy as jnp
from jax import lax
from jax.experimental import pallas as pl
from jax.experimental.pallas import tpu as pltpu
from jax.sharding import PartitionSpec as P

DEPTH = 4
SPAN = 32
MARGIN = 4
ITERS = 4
LANES = 128
MAP_ROWS = 16
INFLATION = 1.1

f32 = jnp.float32
bf16 = jnp.bfloat16
i32 = jnp.int32
VMEM = pl.BlockSpec(memory_space=pltpu.VMEM)
SMEM = pl.BlockSpec(memory_space=pltpu.SMEM)
PARAMS = pltpu.CompilerParams(vmem_limit_bytes=24 * 1024 * 1024)


def iota(shape, dim):
    return lax.broadcasted_iota(i32, shape, dim)


def dot(a, b):
    return jnp.dot(a, b, preferred_element_type=f32)


def one_hot(condition):
    return jnp.where(condition, 1.0, 0.0).astype(bf16)


class Plan:
    def __init__(self, x_shape, count, states):
        self.members, self.states, self.rows, self.cols = x_shape
        self.count = count
        self.total = self.members * count
        self.patches = self.cols // SPAN
        self.bands = self.rows // DEPTH
        self.groups = self.bands // self.patches
        chips = count // 2
        if count % 2 == 0 and chips % self.patches == 0:
            self.place = [
                (2 * (i // 2 // self.patches) + i % 2, i // 2 % self.patches) for i in range(count)
            ]
        else:
            self.place = [(i // self.patches, i % self.patches) for i in range(count)]
        self.slot_bands = self.patches + min(2, self.groups - 1) if self.groups > 1 else self.patches
        self.full = self.slot_bands == self.patches + 2
        self.per_band = self.states + 1
        self.field = self.slot_bands * self.per_band
        self.map_groups = 4 * MAP_ROWS // self.members
        self.slot = self.field + self.map_groups
        self.index_of = {p: i for i, p in enumerate(self.place)}

    def group_of(self, index):
        return sum(jnp.where(index == i, g, 0) for i, (g, _) in enumerate(self.place))

    def shift_of(self, group):
        return jnp.where(group == 0, 0 if self.full else 1, 0)

    def first_band(self, group):
        low = self.patches * group - 1
        return low if self.full else max(low, 0)

    def band_slots(self, band):
        return [
            (g, band - self.first_band(g))
            for g in range(self.groups)
            if 0 <= band - self.first_band(g) < self.slot_bands
        ]


def side_source(lane, column, cols):
    eighth = lane % (2 * MARGIN)
    low = column * SPAN - MARGIN + eighth
    high = column * SPAN + SPAN + eighth - MARGIN
    return jnp.where(eighth < MARGIN, low, high)


def pack_kernel(plan, x_ref, buf_ref, turned, q_ref):
    half = 16
    rows, cols = plan.rows, plan.cols
    span = half * rows
    r = iota((span, span), 0)
    k = iota((span, span), 1)
    perm = one_hot((r % half == k // rows) & (r // half == k % rows))
    for s in range(plan.states):
        for h in range(plan.members // half):
            piece = x_ref[h * half : (h + 1) * half, s].reshape(span, cols)
            turned[s, :, h * half : (h + 1) * half, :] = (
                dot(perm, piece).astype(bf16).reshape(rows, half, cols)
            )
    wide = DEPTH * cols
    r = iota((wide, wide), 0)
    k = iota((wide, wide), 1)
    q_ref[...] = one_hot(
        (r // cols == (k % LANES) // SPAN) & (r % cols == (k // LANES) * SPAN + k % SPAN)
    )
    m = plan.members
    for s in range(plan.states):
        center = dot(banded(plan, turned, s), q_ref[...]).astype(bf16)
        for b in range(plan.bands):
            for c in range(plan.patches):
                value = center[b * m : (b + 1) * m, c * LANES : (c + 1) * LANES]
                for g, position in plan.band_slots(b):
                    buf_ref[plan.index_of[(g, c)], position * plan.states + s] = value
    if plan.full:
        zero = jnp.zeros((plan.members, LANES), bf16)
        for c in range(plan.patches):
            for s in range(plan.states):
                buf_ref[plan.index_of[(0, c)], s] = zero
                last = (plan.slot_bands - 1) * plan.states + s
                buf_ref[plan.index_of[(plan.groups - 1, c)], last] = zero


def banded(plan, turned, s):
    return jnp.concatenate(
        [
            jnp.concatenate([turned[s, b * DEPTH + t] for b in range(plan.bands)], axis=0)
            for t in range(DEPTH)
        ],
        axis=1,
    )


def sides_kernel(plan, turned, own_ref, up_ref, down_ref, side_ref):
    cols = plan.cols
    n_side = (plan.patches + 2) * LANES
    col = iota((cols, n_side), 0)
    out = iota((cols, n_side), 1)
    column = out // LANES
    lane = out % LANES
    eighth = lane % (2 * MARGIN)
    source = side_source(lane, column, cols)
    to_up = (column == plan.patches) & (eighth < MARGIN)
    to_down = (column == plan.patches + 1) & (eighth >= MARGIN)
    source = jnp.where(column < plan.patches, source, -1)
    source = jnp.where(to_up, cols - MARGIN + eighth, source)
    source = jnp.where(to_down, eighth - MARGIN, source)
    hit = jnp.where(col == source, 1.0, 0.0)
    which = iota((1, n_side), 1) % LANES // (2 * MARGIN)
    for s in range(plan.states):
        for t in range(DEPTH):
            at = s * DEPTH + t
            side_ref[at * cols : (at + 1) * cols, :] = jnp.where(which == at, hit, 0.0).astype(bf16)
    lhs = jnp.concatenate([banded(plan, turned, s) for s in range(plan.states)], axis=1)
    sides = dot(lhs, side_ref[...]).astype(bf16)
    for c in range(plan.patches):
        own_ref[c] = sides[:, c * LANES : (c + 1) * LANES]
    at = plan.patches * LANES
    up_ref[...] = sides[:, at : at + LANES]
    down_ref[...] = sides[:, at + LANES : at + 2 * LANES]


def split2(a):
    high = a.astype(bf16)
    return high, (a - high.astype(f32)).astype(bf16)


def window_place(entry):
    height = DEPTH + 2 * MARGIN
    width = SPAN + 2 * MARGIN
    plane = height * width
    state = sum((entry >= plane * n).astype(i32) for n in range(1, 4))
    rest = entry - state * plane
    row = (rest * 1639) >> 16
    col = rest - row * width
    band = row >> 2
    inner = row & 3
    center = (col >= MARGIN) & (col < MARGIN + SPAN)
    eighth = jnp.where(col < MARGIN, col, col - SPAN)
    lane = jnp.where(center, inner * SPAN + col - MARGIN, state * SPAN + inner * 2 * MARGIN + eighth)
    group = jnp.where(center, band * 4 + state, 12 + band)
    return group, lane


def map_kernel(patches, table, count_ref, factor_ref, cell_ref, class_ref, value_ref, inv_ref, out_ref):
    slots = cell_ref.shape[1]
    group, lane = window_place(cell_ref[...])
    classes = class_ref[...]
    factor = jnp.zeros(classes.shape, f32)
    for n in range(table):
        factor = jnp.where(classes == n, factor_ref[n], factor)
    weight = inv_ref[...] * factor
    order = iota((1, slots), 1)
    for p in range(patches):
        live = jnp.where(order < count_ref[0, p], weight[p : p + 1], 0.0)
        hot = one_hot(iota((LANES, slots), 0) == lane[p : p + 1])
        pick = iota((MAP_ROWS, slots), 0) == group[p : p + 1]
        parts = []
        for source in (live, live * value_ref[p : p + 1]):
            for _ in range(3):
                high = source.astype(bf16).astype(f32)
                parts.append(jnp.where(pick, high, 0.0).astype(bf16))
                source = source - high
        maps = lax.dot_general(
            jnp.concatenate(parts, axis=0), hot, (((1,), (1,)), ((), ())), preferred_element_type=f32
        )
        n = MAP_ROWS
        w_high, w_low = split2(maps[:n] + maps[n : 2 * n] + maps[2 * n : 3 * n])
        v_high, v_low = split2(maps[3 * n : 4 * n] + maps[4 * n : 5 * n] + maps[5 * n :])
        out_ref[p] = jnp.concatenate([w_high, w_low, v_high, v_low], axis=0)


def join_kernel(plan, place_ref, own_ref, maps_ref, left_ref, right_ref, *outs):
    buf_ref = outs[-1]
    index = place_ref[0]
    m = plan.members
    zero = jnp.zeros((m, LANES), bf16)
    for b in range(plan.bands):
        at = slice(b * m, (b + 1) * m)
        for c in range(plan.patches):
            value = own_ref[c, at]
            if c == 0:
                value = value + left_ref[at]
            if c == plan.patches - 1:
                value = value + right_ref[at]
            for g, position in plan.band_slots(b):
                buf_ref[plan.index_of[(g, c)], position] = value
    if plan.full:
        for c in range(plan.patches):
            buf_ref[plan.index_of[(0, c)], 0] = zero
            buf_ref[plan.index_of[(plan.groups - 1, c)], plan.slot_bands - 1] = zero
    for i, (g, c) in enumerate(plan.place):
        piece = jnp.where(index // plan.patches == g, maps_ref[c], jnp.zeros_like(maps_ref[c]))
        for n in range(plan.map_groups):
            buf_ref[i, plan.slot_bands + n] = piece[n * m : (n + 1) * m]
    for k in range(plan.count):
        outs[k][...] = buf_ref[index ^ k]


def mm3(ah, al, bh, bl):
    return dot(jnp.concatenate([ah, ah, al], axis=1), jnp.concatenate([bh, bl, bh], axis=0))


def center_of(plan, shift, fields, bands_at, width, xs, avgs):
    sources = fields.shape[0]
    total, patches = plan.total, plan.patches
    step = 8 if width > 1 else 1
    if not plan.full:
        edges = (0, patches + 1)
        if plan.slot_bands > patches:
            edges = (jnp.where(shift == 1, 0, patches + 1),)
        for edge in edges:
            lanes = pl.ds(edge * width * LANES, width * LANES)
            if not isinstance(edge, int):
                lanes = pl.ds(pl.multiple_of(edge * width * LANES, LANES), width * LANES)
            xs[:, lanes] = jnp.zeros((total, width * LANES), bf16)
            avgs[pl.ds(edge * step, step)] = jnp.zeros((step, LANES), f32)
    for b in range(plan.slot_bands):
        means = []
        for inner in range(width):
            at = bands_at + b * width + inner
            raw = jnp.concatenate([fields[n, at] for n in range(sources)], axis=0).astype(f32)
            mean = jnp.sum(raw, axis=0, keepdims=True) / total
            means.append(mean)
            lanes = pl.multiple_of(((shift + b) * width + inner) * LANES, LANES)
            xs[:, pl.ds(lanes, LANES)] = (raw - mean).astype(bf16)
        if width > 1:
            means.append(jnp.zeros((step - width, LANES), f32))
        avgs[pl.ds((b + shift) * step, step)] = jnp.concatenate(means, axis=0)


def center_kernel(plan, place_ref, x_ref, xs, avgs):
    shift = plan.shift_of(plan.group_of(place_ref[0]))
    center_of(plan, shift, x_ref, 0, plan.states, xs, avgs)


def analyse_kernel(
    plan, relative, place_ref, xs, avgs, *rest
):
    *pieces, out_ref, side_xs, side_avgs, scaled, lead, gathered = rest

    total, states, patches = plan.total, plan.states, plan.patches
    sources, _, piece_rows, _ = out_ref.shape
    group = plan.group_of(place_ref[0])
    if relative:
        for k in range(plan.count):
            gathered[place_ref[0] ^ k] = pieces[k][...]
        side_ref, maps_ref, map_at = gathered, gathered, plan.slot_bands
    else:
        (side_ref, maps_ref), map_at = pieces, 0
    center_of(plan, plan.shift_of(group), side_ref, 0, 1, side_xs, side_avgs)
    eye = jnp.where(iota((total, total), 0) == iota((total, total), 1), 1.0, 0.0)
    grams, forcings, norms = [], [], []
    for q in range(patches):
        n_map = maps_ref.shape[1] - map_at
        maps = jnp.concatenate(
            [maps_ref[patches * group + q, map_at + n] for n in range(n_map)], axis=0
        ).astype(f32)
        n = MAP_ROWS
        weight = maps[:n] + maps[n : 2 * n]
        value = maps[2 * n : 3 * n] + maps[3 * n :]
        lead[...] = jnp.zeros_like(lead)
        for at in range(3 * (states + 1)):
            if at < 3 * states:
                lanes = (q * states + at) * LANES
                source = xs[:, lanes : lanes + LANES]
                row = (q + at // states) * 8 + at % states
                mean = avgs[row : row + 1]
            else:
                row = q + at - 3 * states
                source = side_xs[:, row * LANES : (row + 1) * LANES]
                mean = side_avgs[row : row + 1]
            w = weight[at : at + 1]
            here = slice(at * LANES, (at + 1) * LANES)
            scaled[q, :total, here] = (source.astype(f32) * w).astype(bf16)
            v = value[at : at + 1] - w * mean
            for part in range(3):
                high = v.astype(bf16).astype(f32)
                lead[part : part + 1, here] = high
                v = v - high
        scaled[q, total:] = lead[...].astype(bf16)
        first = q * states * LANES
        window = jnp.concatenate(
            [
                xs[:, first : first + 3 * states * LANES],
                side_xs[:, q * LANES : (q + 3) * LANES],
            ],
            axis=1,
        )
        both = lax.dot_general(
            scaled[q], window, (((1,), (1,)), ((), ())), preferred_element_type=f32
        )
        gram = both[:total] + ((total - 1) / INFLATION) * eye
        forcings.append(both[total : total + 1] + both[total + 1 : total + 2] + both[total + 2 : total + 3])
        norm = jnp.sqrt(jnp.sum(jnp.sum(gram * gram, axis=1, keepdims=True), axis=0, keepdims=True))
        norms.append(norm)
        grams.append(gram / norm)
    factors, iterates, roots = [], [], []
    for q in range(patches):
        y = split2(grams[q])
        f = split2(1.5 * eye - 0.5 * grams[q])
        iterates.append(split2(mm3(*y, *f)))
        roots.append(f)
    for sweep in range(1, ITERS):
        for q in range(patches):
            f = split2(1.5 * eye - 0.5 * mm3(*roots[q], *iterates[q]))
            if sweep + 1 < ITERS:
                iterates[q] = split2(mm3(*iterates[q], *f))
                roots[q] = split2(mm3(*roots[q], *f))
            else:
                roots[q] = mm3(*roots[q], *f)
    for q in range(patches):
        root = roots[q]
        force = jnp.broadcast_to(forcings[q], (8, total))
        part = jnp.dot(force, root, precision=lax.Precision.HIGHEST, preferred_element_type=f32)
        move = jnp.dot(part, root, precision=lax.Precision.HIGHEST, preferred_element_type=f32)
        move = move[:1] / norms[q]
        transform = (jnp.sqrt((total - 1.0) / norms[q]) * root + move).astype(bf16)
        first = (q + 1) * states * LANES
        analysed = dot(transform, xs[:, first : first + states * LANES])
        for s in range(states):
            row = (q + 1) * 8 + s
            value = (analysed[:, s * LANES : (s + 1) * LANES] + avgs[row : row + 1]).astype(bf16)
            for n in range(sources):
                out_ref[n, q * states + s] = value[n * piece_rows : (n + 1) * piece_rows]


def unpack_kernel(plan, in_ref, out_ref, q_ref, turned):
    half = 16
    m, rows, cols, states = plan.members, plan.rows, plan.cols, plan.states
    wide = DEPTH * cols
    r = iota((wide, wide), 0)
    k = iota((wide, wide), 1)
    q_ref[...] = one_hot(
        (k // cols == (r % LANES) // SPAN) & (k % cols == (r // LANES) * SPAN + r % SPAN)
    )
    for s in range(states):
        lhs = []
        for b in range(plan.bands):
            g, q = b // plan.patches, b % plan.patches
            lhs.append(
                jnp.concatenate(
                    [in_ref[plan.index_of[(g, c)], q * states + s] for c in range(plan.patches)], axis=1
                )
            )
        opened = dot(jnp.concatenate(lhs, axis=0), q_ref[...]).astype(bf16)
        for b in range(plan.bands):
            for t in range(DEPTH):
                turned[s, b * DEPTH + t] = opened[b * m : (b + 1) * m, t * cols : (t + 1) * cols]
    span = half * rows
    r = iota((span, span), 0)
    k = iota((span, span), 1)
    perm = one_hot((k % half == r // rows) & (k // half == r % rows))
    for s in range(states):
        for h in range(m // half):
            piece = turned[s, :, h * half : (h + 1) * half, :].reshape(span, cols)
            out_ref[h * half : (h + 1) * half, s] = (
                dot(perm, piece).astype(bf16).reshape(half, rows, cols)
            )


def shifts(axis):
    count = lax.axis_size(axis)
    forward = [(i, i + 1) for i in range(count - 1)]
    return forward, [(b, a) for a, b in forward]


def pack_plain(plan, x):
    m, s, b = plan.members, plan.states, plan.bands
    bands = x.reshape(m, s, b, DEPTH, plan.cols)
    center = bands.reshape(m, s, b, DEPTH, plan.patches, SPAN).transpose(4, 2, 1, 0, 3, 5)
    center = center.reshape(plan.patches, b, s, m, LANES)
    padded = jnp.pad(bands, ((0, 0),) * 4 + ((MARGIN, MARGIN),))
    sides = jnp.stack(
        [
            jnp.concatenate(
                [
                    padded[..., c * SPAN : c * SPAN + MARGIN],
                    padded[..., (c + 1) * SPAN + MARGIN : (c + 1) * SPAN + 2 * MARGIN],
                ],
                axis=-1,
            )
            for c in range(plan.patches)
        ]
    )
    sides = sides.transpose(0, 3, 1, 2, 4, 5).reshape(plan.patches, b, 1, m, LANES)
    center, sides = (jnp.pad(a, ((0, 0), (1, 1)) + ((0, 0),) * 3) for a in (center, sides))
    slots, side_slots = [], []
    for g, c in plan.place:
        at = slice(plan.first_band(g) + 1, plan.first_band(g) + 1 + plan.slot_bands)
        slots.append(center[c, at].reshape(-1, m, LANES))
        side_slots.append(jnp.pad(sides[c, at, 0], ((0, plan.map_groups), (0, 0), (0, 0))))
    empty = jnp.zeros_like(bands[..., :MARGIN])
    strips = []
    for pair in ((bands[..., -MARGIN:], empty), (empty, bands[..., :MARGIN])):
        strip = jnp.concatenate(pair, axis=-1).transpose(2, 0, 1, 3, 4)
        strips.append(strip.reshape(b * m, LANES))
    return jnp.stack(slots), jnp.stack(side_slots), strips[0], strips[1]


def unpack_plain(plan, arrived):
    m, s, b = plan.members, plan.states, plan.bands
    bands = []
    for band in range(b):
        g, q = band // plan.patches, band % plan.patches
        pieces = jnp.stack(
            [arrived[plan.index_of[(g, c)], q * s : (q + 1) * s] for c in range(plan.patches)]
        )
        pieces = pieces.reshape(plan.patches, s, m, DEPTH, SPAN).transpose(2, 1, 3, 0, 4)
        bands.append(pieces.reshape(m, s, DEPTH, plan.cols))
    return jnp.concatenate(bands, axis=2)


def local(x, tally, cells, classes, readings, inverse, factors):
    count = lax.axis_size("mem")
    plan = Plan(x.shape, count, x.shape[1])
    patches = plan.patches
    index = lax.axis_index("mem")
    where = index.reshape(1)
    aligned = plan.members % 16 == 0
    states, members, total = plan.states, plan.members, plan.total
    strip = (plan.bands * members, LANES)
    side_slot = (count, plan.slot_bands + plan.map_groups, members, LANES)
    center_groups = plan.slot_bands * states
    if aligned:
        packed, turned = pl.pallas_call(
            functools.partial(pack_kernel, plan),
            out_shape=(
                jax.ShapeDtypeStruct((count, center_groups, members, LANES), bf16),
                jax.ShapeDtypeStruct((states, plan.rows, members, plan.cols), bf16),
            ),
            in_specs=[VMEM],
            out_specs=(VMEM, VMEM),
            scratch_shapes=[pltpu.VMEM((DEPTH * plan.cols, DEPTH * plan.cols), bf16)],
            compiler_params=PARAMS,
            name="pack",
        )(x)
    else:
        packed, side_slots, upward, downward = pack_plain(plan, x)
    centers = lax.all_to_all(packed, "mem", split_axis=0, concat_axis=0, tiled=True)
    if aligned:
        own, upward, downward = pl.pallas_call(
            functools.partial(sides_kernel, plan),
            out_shape=(
                jax.ShapeDtypeStruct((patches,) + strip, bf16),
                jax.ShapeDtypeStruct(strip, bf16),
                jax.ShapeDtypeStruct(strip, bf16),
            ),
            in_specs=[VMEM],
            out_specs=(VMEM, VMEM, VMEM),
            scratch_shapes=[
                pltpu.VMEM((states * DEPTH * plan.cols, (patches + 2) * LANES), bf16),
            ],
            compiler_params=PARAMS,
            name="sides",
        )(turned)
    forward, backward = shifts("col")
    left = lax.ppermute(upward, "col", forward)
    right = lax.ppermute(downward, "col", backward)
    slots = cells.shape[-1]
    maps = pl.pallas_call(
        functools.partial(map_kernel, patches, factors.shape[0]),
        out_shape=jax.ShapeDtypeStruct((patches, 4 * MAP_ROWS, LANES), bf16),
        in_specs=[SMEM, SMEM, VMEM, VMEM, VMEM, VMEM],
        out_specs=VMEM,
        compiler_params=PARAMS,
        name="maps",
    )(
        tally,
        factors,
        cells.reshape(patches, slots),
        classes.reshape(patches, slots),
        readings.reshape(patches, slots),
        inverse.reshape(patches, slots),
    )
    if aligned:
        parts = pl.pallas_call(
            functools.partial(join_kernel, plan),
            out_shape=(jax.ShapeDtypeStruct(side_slot[1:], bf16),) * count,
            in_specs=[SMEM, VMEM, VMEM, VMEM, VMEM],
            out_specs=(VMEM,) * count,
            scratch_shapes=[pltpu.VMEM(side_slot, bf16)],
            compiler_params=PARAMS,
            name="join",
        )(where, own, maps, left, right)
        arrived = [parts[0]] + [
            lax.ppermute(parts[k], "mem", [(i, i ^ k) for i in range(count)]) for k in range(1, count)
        ]
    else:
        for b in range(plan.bands):
            at = slice(b * members, (b + 1) * members)
            for column, extra in ((0, left[at]), (patches - 1, right[at])):
                for g, position in plan.band_slots(b):
                    side_slots = side_slots.at[plan.index_of[(g, column)], position].add(extra)
        for i, (g, c) in enumerate(plan.place):
            piece = jnp.where(index // patches == g, maps[c], 0).reshape(-1, members, LANES)
            side_slots = side_slots.at[i, plan.slot_bands :].set(piece)
        arrived = lax.all_to_all(side_slots, "mem", split_axis=0, concat_axis=0, tiled=True)
        centers, sides = (
            a.transpose(1, 0, 2, 3).reshape(1, -1, total, LANES)
            for a in (centers, arrived[:, : plan.slot_bands])
        )
        arrived = [sides, arrived[:, plan.slot_bands :].reshape(count, 1, 4 * MAP_ROWS, LANES)]
    pieces = (count, members) if aligned else (1, total)
    bands = patches + 2
    center_xs, center_avgs = pl.pallas_call(
        functools.partial(center_kernel, plan),
        out_shape=(
            jax.ShapeDtypeStruct((total, bands * states * LANES), bf16),
            jax.ShapeDtypeStruct((bands * 8, LANES), f32),
        ),
        in_specs=[SMEM, VMEM],
        out_specs=(VMEM, VMEM),
        compiler_params=PARAMS,
        name="center",
    )(where, centers)
    depth = 3 * (states + 1) * LANES
    analysed = pl.pallas_call(
        functools.partial(analyse_kernel, plan, aligned),
        out_shape=jax.ShapeDtypeStruct((pieces[0], patches * states, pieces[1], LANES), bf16),
        in_specs=[SMEM, VMEM, VMEM] + [VMEM] * len(arrived),
        out_specs=VMEM,
        scratch_shapes=[
            pltpu.VMEM((total, bands * LANES), bf16),
            pltpu.VMEM((8, LANES), f32),
            pltpu.VMEM((patches, total + 16, depth), bf16),
            pltpu.VMEM((16, depth), f32),
            pltpu.VMEM(side_slot if aligned else (8, LANES), bf16),
        ],
        compiler_params=PARAMS,
        name="analyse",
    )(where, center_xs, center_avgs, *arrived)
    if not aligned:
        analysed = analysed.reshape(-1, count, plan.members, LANES).transpose(1, 0, 2, 3)
    returned = lax.all_to_all(analysed, "mem", split_axis=0, concat_axis=0, tiled=True)
    if not aligned:
        return unpack_plain(plan, returned)
    return pl.pallas_call(
        functools.partial(unpack_kernel, plan),
        out_shape=jax.ShapeDtypeStruct(x.shape, bf16),
        in_specs=[VMEM],
        out_specs=VMEM,
        scratch_shapes=[
            pltpu.VMEM((DEPTH * plan.cols, DEPTH * plan.cols), bf16),
            pltpu.VMEM((plan.states, plan.rows, plan.members, plan.cols), bf16),
        ],
        compiler_params=PARAMS,
        name="unpack",
    )(returned)


def solution(mesh):
    placed = (
        P("mem", None, None, "col"),
        P("mem", "col"),
        P("mem", "col", None),
        P("mem", "col", None),
        P("mem", "col", None),
        P("mem", "col", None),
        P(),
    )
    return jax.shard_map(
        local, mesh=mesh, in_specs=placed, out_specs=P("mem", None, None, "col"), check_vma=False
    )
```

```python
import functools
import jax
import jax.numpy as jnp
from jax import lax
from jax.experimental import pallas as pl
from jax.experimental.pallas import tpu as pltpu
from jax.sharding import PartitionSpec as P

DEPTH = 4
SPAN = 32
MARGIN = 4
ITERS = 4
LANES = 128
HALF = 16
MAP_ROWS = 16
INFLATION = 1.1

f32 = jnp.float32
bf16 = jnp.bfloat16
i32 = jnp.int32
VMEM = pl.BlockSpec(memory_space=pltpu.VMEM)
SMEM = pl.BlockSpec(memory_space=pltpu.SMEM)
PARAMS = pltpu.CompilerParams(vmem_limit_bytes=14 * 1024 * 1024)


def iota(shape, dim):
    return lax.broadcasted_iota(i32, shape, dim)


def dot(a, b):
    return jnp.dot(a, b, preferred_element_type=f32)


def one_hot(condition):
    return jnp.where(condition, 1.0, 0.0).astype(bf16)


class Plan:
    def __init__(self, x_shape, count, states):
        self.members, self.states, self.rows, self.cols = x_shape
        self.count = count
        self.total = self.members * count
        self.patches = self.cols // SPAN
        self.bands = self.rows // DEPTH
        self.groups = self.bands // self.patches
        chips = count // 2
        if count % 2 == 0 and chips % self.patches == 0:
            self.place = [
                (2 * (i // 2 // self.patches) + i % 2, i // 2 % self.patches) for i in range(count)
            ]
        else:
            self.place = [(i // self.patches, i % self.patches) for i in range(count)]
        self.slot_bands = self.patches + min(2, self.groups - 1) if self.groups > 1 else self.patches
        self.full = self.slot_bands == self.patches + 2
        self.per_band = self.states + 1
        self.field = self.slot_bands * self.per_band
        self.map_groups = 4 * MAP_ROWS // self.members
        self.slot = self.field + self.map_groups
        self.index_of = {p: i for i, p in enumerate(self.place)}

    def group_of(self, index):
        return sum(jnp.where(index == i, g, 0) for i, (g, _) in enumerate(self.place))

    def shift_of(self, group):
        return jnp.where(group == 0, 0 if self.full else 1, 0)

    def first_band(self, group):
        low = self.patches * group - 1
        return low if self.full else max(low, 0)

    def band_slots(self, band):
        return [
            (g, band - self.first_band(g))
            for g in range(self.groups)
            if 0 <= band - self.first_band(g) < self.slot_bands
        ]


def side_source(lane, column, cols):
    eighth = lane % (2 * MARGIN)
    low = column * SPAN - MARGIN + eighth
    high = column * SPAN + SPAN + eighth - MARGIN
    return jnp.where(eighth < MARGIN, low, high)


def turn_table():
    r = iota((HALF * HALF, HALF * HALF), 0)
    k = iota((HALF * HALF, HALF * HALF), 1)
    return one_hot((r % HALF == k // HALF) & (r // HALF == k % HALF))


def lane_table(cols, closing):
    wide = DEPTH * cols
    r = iota((wide, wide), 0 if closing else 1)
    k = iota((wide, wide), 1 if closing else 0)
    return one_hot(
        (r // cols == (k % LANES) // SPAN) & (r % cols == (k // LANES) * SPAN + k % SPAN)
    )


def turn(table, read, write, first, second):
    for a in range(0, first, HALF):
        for b in range(0, second, 2 * HALF):
            pair = [read(a, b + n * HALF).reshape(HALF * HALF, LANES) for n in range(2)]
            done = dot(table, jnp.concatenate(pair, axis=1)).astype(bf16)
            for n in range(2):
                piece = done[:, n * LANES : (n + 1) * LANES]
                write(a, b + n * HALF, piece.reshape(HALF, HALF, LANES))


def tables_kernel(plan, turn_ref, close_ref):
    turn_ref[...] = turn_table()
    close_ref[...] = lane_table(plan.cols, True)


def pack_kernel(plan, x_ref, turn_ref, close_ref, buf_ref, turned):
    table = turn_ref[...]
    m = plan.members
    for s in range(plan.states):
        def read(a, b):
            return x_ref[a : a + HALF, s, b : b + HALF]

        def write(a, b, piece):
            turned[s, b : b + HALF, a : a + HALF] = piece

        turn(table, read, write, m, plan.rows)
        center = dot(banded(plan, turned, s), close_ref[...]).astype(bf16)
        for b in range(plan.bands):
            for c in range(plan.patches):
                value = center[b * m : (b + 1) * m, c * LANES : (c + 1) * LANES]
                for g, position in plan.band_slots(b):
                    buf_ref[plan.index_of[(g, c)], position * plan.states + s] = value
    if plan.full:
        zero = jnp.zeros((plan.members, LANES), bf16)
        for c in range(plan.patches):
            for s in range(plan.states):
                buf_ref[plan.index_of[(0, c)], s] = zero
                last = (plan.slot_bands - 1) * plan.states + s
                buf_ref[plan.index_of[(plan.groups - 1, c)], last] = zero


def banded(plan, turned, s):
    return jnp.concatenate(
        [
            jnp.concatenate([turned[s, b * DEPTH + t] for b in range(plan.bands)], axis=0)
            for t in range(DEPTH)
        ],
        axis=1,
    )


def sides_kernel(plan, turned, own_ref, up_ref, down_ref, side_ref):
    cols = plan.cols
    n_side = (plan.patches + 2) * LANES
    col = iota((cols, n_side), 0)
    out = iota((cols, n_side), 1)
    column = out // LANES
    lane = out % LANES
    eighth = lane % (2 * MARGIN)
    source = side_source(lane, column, cols)
    to_up = (column == plan.patches) & (eighth < MARGIN)
    to_down = (column == plan.patches + 1) & (eighth >= MARGIN)
    source = jnp.where(column < plan.patches, source, -1)
    source = jnp.where(to_up, cols - MARGIN + eighth, source)
    source = jnp.where(to_down, eighth - MARGIN, source)
    hit = jnp.where(col == source, 1.0, 0.0)
    which = iota((1, n_side), 1) % LANES // (2 * MARGIN)
    for s in range(plan.states):
        for t in range(DEPTH):
            at = s * DEPTH + t
            side_ref[at * cols : (at + 1) * cols, :] = jnp.where(which == at, hit, 0.0).astype(bf16)
    lhs = jnp.concatenate([banded(plan, turned, s) for s in range(plan.states)], axis=1)
    sides = dot(lhs, side_ref[...]).astype(bf16)
    for c in range(plan.patches):
        own_ref[c] = sides[:, c * LANES : (c + 1) * LANES]
    at = plan.patches * LANES
    up_ref[...] = sides[:, at : at + LANES]
    down_ref[...] = sides[:, at + LANES : at + 2 * LANES]


def split2(a):
    high = a.astype(bf16)
    return high, (a - high.astype(f32)).astype(bf16)


def window_place(entry):
    height = DEPTH + 2 * MARGIN
    width = SPAN + 2 * MARGIN
    plane = height * width
    state = sum((entry >= plane * n).astype(i32) for n in range(1, 4))
    rest = entry - state * plane
    row = (rest * 1639) >> 16
    col = rest - row * width
    band = row >> 2
    inner = row & 3
    center = (col >= MARGIN) & (col < MARGIN + SPAN)
    eighth = jnp.where(col < MARGIN, col, col - SPAN)
    lane = jnp.where(center, inner * SPAN + col - MARGIN, state * SPAN + inner * 2 * MARGIN + eighth)
    group = jnp.where(center, band * 4 + state, 12 + band)
    return group, lane


def map_kernel(patches, table, count_ref, factor_ref, cell_ref, class_ref, value_ref, inv_ref, out_ref):
    slots = cell_ref.shape[1]
    group, lane = window_place(cell_ref[...])
    classes = class_ref[...]
    factor = jnp.zeros(classes.shape, f32)
    for n in range(table):
        factor = jnp.where(classes == n, factor_ref[n], factor)
    weight = inv_ref[...] * factor
    order = iota((1, slots), 1)
    for p in range(patches):
        live = jnp.where(order < count_ref[0, p], weight[p : p + 1], 0.0)
        hot = one_hot(iota((LANES, slots), 0) == lane[p : p + 1])
        pick = iota((MAP_ROWS, slots), 0) == group[p : p + 1]
        parts = []
        for source in (live, live * value_ref[p : p + 1]):
            for _ in range(3):
                high = source.astype(bf16).astype(f32)
                parts.append(jnp.where(pick, high, 0.0).astype(bf16))
                source = source - high
        maps = lax.dot_general(
            jnp.concatenate(parts, axis=0), hot, (((1,), (1,)), ((), ())), preferred_element_type=f32
        )
        n = MAP_ROWS
        w_high, w_low = split2(maps[:n] + maps[n : 2 * n] + maps[2 * n : 3 * n])
        v_high, v_low = split2(maps[3 * n : 4 * n] + maps[4 * n : 5 * n] + maps[5 * n :])
        out_ref[p] = jnp.concatenate([w_high, w_low, v_high, v_low], axis=0)


def join_kernel(plan, place_ref, own_ref, maps_ref, left_ref, right_ref, *outs):
    buf_ref = outs[-1]
    index = place_ref[0]
    m = plan.members
    zero = jnp.zeros((m, LANES), bf16)
    for b in range(plan.bands):
        at = slice(b * m, (b + 1) * m)
        for c in range(plan.patches):
            value = own_ref[c, at]
            if c == 0:
                value = value + left_ref[at]
            if c == plan.patches - 1:
                value = value + right_ref[at]
            for g, position in plan.band_slots(b):
                buf_ref[plan.index_of[(g, c)], position] = value
    if plan.full:
        for c in range(plan.patches):
            buf_ref[plan.index_of[(0, c)], 0] = zero
            buf_ref[plan.index_of[(plan.groups - 1, c)], plan.slot_bands - 1] = zero
    for i, (g, c) in enumerate(plan.place):
        piece = jnp.where(index // plan.patches == g, maps_ref[c], jnp.zeros_like(maps_ref[c]))
        for n in range(plan.map_groups):
            buf_ref[i, plan.slot_bands + n] = piece[n * m : (n + 1) * m]
    for k in range(plan.count):
        outs[k][...] = buf_ref[index ^ k]


def mm2(a, b):
    return dot(jnp.concatenate(split2(a), axis=1), jnp.concatenate([b, b], axis=0))


def center_of(plan, shift, fields, bands_at, width, xs, avgs):
    sources = fields.shape[0]
    total, patches = plan.total, plan.patches
    step = 8 if width > 1 else 1
    if not plan.full:
        edges = (0, patches + 1)
        if plan.slot_bands > patches:
            edges = (jnp.where(shift == 1, 0, patches + 1),)
        for edge in edges:
            lanes = pl.ds(edge * width * LANES, width * LANES)
            if not isinstance(edge, int):
                lanes = pl.ds(pl.multiple_of(edge * width * LANES, LANES), width * LANES)
            xs[:, lanes] = jnp.zeros((total, width * LANES), bf16)
            avgs[pl.ds(edge * step, step)] = jnp.zeros((step, LANES), f32)
    for b in range(plan.slot_bands):
        means = []
        for inner in range(width):
            at = bands_at + b * width + inner
            raw = jnp.concatenate([fields[n, at] for n in range(sources)], axis=0).astype(f32)
            mean = jnp.sum(raw, axis=0, keepdims=True) / total
            means.append(mean)
            lanes = pl.multiple_of(((shift + b) * width + inner) * LANES, LANES)
            xs[:, pl.ds(lanes, LANES)] = (raw - mean).astype(bf16)
        if width > 1:
            means.append(jnp.zeros((step - width, LANES), f32))
        avgs[pl.ds((b + shift) * step, step)] = jnp.concatenate(means, axis=0)


def center_kernel(plan, place_ref, x_ref, xs, avgs, turn_ref=None, open_ref=None):
    if open_ref is not None:
        turn_ref[...] = turn_table()
        open_ref[...] = lane_table(plan.cols, False)
    shift = plan.shift_of(plan.group_of(place_ref[0]))
    center_of(plan, shift, x_ref, 0, plan.states, xs, avgs)


def analyse_kernel(
    plan, relative, place_ref, xs, avgs, *rest
):
    *pieces, out_ref, side_xs, side_avgs, scaled, lead, gathered = rest

    total, states, patches = plan.total, plan.states, plan.patches
    sources, _, piece_rows, _ = out_ref.shape
    group = plan.group_of(place_ref[0])
    if relative:
        for k in range(plan.count):
            gathered[place_ref[0] ^ k] = pieces[k][...]
        side_ref, maps_ref, map_at = gathered, gathered, plan.slot_bands
    else:
        (side_ref, maps_ref), map_at = pieces, 0
    center_of(plan, plan.shift_of(group), side_ref, 0, 1, side_xs, side_avgs)
    eye = jnp.where(iota((total, total), 0) == iota((total, total), 1), 1.0, 0.0)
    grams, forcings, norms = [], [], []
    for q in range(patches):
        n_map = maps_ref.shape[1] - map_at
        maps = jnp.concatenate(
            [maps_ref[patches * group + q, map_at + n] for n in range(n_map)], axis=0
        ).astype(f32)
        n = MAP_ROWS
        weight = maps[:n] + maps[n : 2 * n]
        value = maps[2 * n : 3 * n] + maps[3 * n :]
        lead[...] = jnp.zeros_like(lead)
        for at in range(3 * (states + 1)):
            if at < 3 * states:
                lanes = (q * states + at) * LANES
                source = xs[:, lanes : lanes + LANES]
                row = (q + at // states) * 8 + at % states
                mean = avgs[row : row + 1]
            else:
                row = q + at - 3 * states
                source = side_xs[:, row * LANES : (row + 1) * LANES]
                mean = side_avgs[row : row + 1]
            w = weight[at : at + 1]
            here = slice(at * LANES, (at + 1) * LANES)
            scaled[q, :total, here] = (source.astype(f32) * w).astype(bf16)
            v = value[at : at + 1] - w * mean
            for part in range(3):
                high = v.astype(bf16).astype(f32)
                lead[part : part + 1, here] = high
                v = v - high
        scaled[q, total:] = lead[...].astype(bf16)
        first = q * states * LANES
        window = jnp.concatenate(
            [
                xs[:, first : first + 3 * states * LANES],
                side_xs[:, q * LANES : (q + 3) * LANES],
            ],
            axis=1,
        )
        both = lax.dot_general(
            scaled[q], window, (((1,), (1,)), ((), ())), preferred_element_type=f32
        )
        gram = both[:total] + ((total - 1) / INFLATION) * eye
        forcings.append(both[total : total + 1] + both[total + 1 : total + 2] + both[total + 2 : total + 3])
        norm = jnp.sqrt(jnp.sum(jnp.sum(gram * gram, axis=1, keepdims=True), axis=0, keepdims=True))
        norms.append(norm)
        grams.append(gram / norm)
    scale = 1.5
    iterates, rests = [], []
    for q in range(patches):
        iterates.append(1.5 * grams[q] - 0.5 * mm2(grams[q], grams[q].astype(bf16)))
        rests.append(-0.5 * grams[q])
    for sweep in range(1, ITERS):
        last = sweep + 1 == ITERS
        for q in range(patches):
            y = iterates[q].astype(bf16)
            product = scale * iterates[q] + mm2(rests[q], y)
            rest = rests[q].astype(bf16)
            both = mm2(product, rest if last else jnp.concatenate([rest, y], axis=1))
            rests[q] = 1.5 * rests[q] - 0.5 * (scale * product + both[:, :total])
            if not last:
                iterates[q] = 1.5 * iterates[q] - 0.5 * both[:, total:]
        scale = scale * 1.5
    roots = [scale * eye + rest for rest in rests]
    for q in range(patches):
        root = roots[q]
        force = jnp.broadcast_to(forcings[q], (8, total))
        high, low = split2(root)
        tall = jnp.concatenate([high, high, low], axis=0)

        def apply(v):
            h, l = split2(v)
            return dot(jnp.concatenate([h, l, h], axis=1), tall)

        move = apply(apply(force))
        move = move[:1] / norms[q]
        transform = (jnp.sqrt((total - 1.0) / norms[q]) * root + move).astype(bf16)
        first = (q + 1) * states * LANES
        analysed = dot(transform, xs[:, first : first + states * LANES])
        for s in range(states):
            row = (q + 1) * 8 + s
            value = (analysed[:, s * LANES : (s + 1) * LANES] + avgs[row : row + 1]).astype(bf16)
            for n in range(sources):
                out_ref[n, q * states + s] = value[n * piece_rows : (n + 1) * piece_rows]


def unpack_kernel(plan, in_ref, turn_ref, open_ref, out_ref, turned):
    m, rows, cols, states = plan.members, plan.rows, plan.cols, plan.states
    table = turn_ref[...]
    for s in range(states):
        lhs = []
        for b in range(plan.bands):
            g, q = b // plan.patches, b % plan.patches
            lhs.append(
                jnp.concatenate(
                    [in_ref[plan.index_of[(g, c)], q * states + s] for c in range(plan.patches)], axis=1
                )
            )
        opened = dot(jnp.concatenate(lhs, axis=0), open_ref[...]).astype(bf16)
        for b in range(plan.bands):
            for t in range(DEPTH):
                turned[s, b * DEPTH + t] = opened[b * m : (b + 1) * m, t * cols : (t + 1) * cols]

        def read(a, b):
            return turned[s, a : a + HALF, b : b + HALF]

        def write(a, b, piece):
            out_ref[b : b + HALF, s, a : a + HALF] = piece

        turn(table, read, write, rows, m)


def shifts(axis):
    count = lax.axis_size(axis)
    forward = [(i, i + 1) for i in range(count - 1)]
    return forward, [(b, a) for a, b in forward]


def pack_plain(plan, x):
    m, s, b = plan.members, plan.states, plan.bands
    bands = x.reshape(m, s, b, DEPTH, plan.cols)
    center = bands.reshape(m, s, b, DEPTH, plan.patches, SPAN).transpose(4, 2, 1, 0, 3, 5)
    center = center.reshape(plan.patches, b, s, m, LANES)
    padded = jnp.pad(bands, ((0, 0),) * 4 + ((MARGIN, MARGIN),))
    sides = jnp.stack(
        [
            jnp.concatenate(
                [
                    padded[..., c * SPAN : c * SPAN + MARGIN],
                    padded[..., (c + 1) * SPAN + MARGIN : (c + 1) * SPAN + 2 * MARGIN],
                ],
                axis=-1,
            )
            for c in range(plan.patches)
        ]
    )
    sides = sides.transpose(0, 3, 1, 2, 4, 5).reshape(plan.patches, b, 1, m, LANES)
    center, sides = (jnp.pad(a, ((0, 0), (1, 1)) + ((0, 0),) * 3) for a in (center, sides))
    slots, side_slots = [], []
    for g, c in plan.place:
        at = slice(plan.first_band(g) + 1, plan.first_band(g) + 1 + plan.slot_bands)
        slots.append(center[c, at].reshape(-1, m, LANES))
        side_slots.append(jnp.pad(sides[c, at, 0], ((0, plan.map_groups), (0, 0), (0, 0))))
    empty = jnp.zeros_like(bands[..., :MARGIN])
    strips = []
    for pair in ((bands[..., -MARGIN:], empty), (empty, bands[..., :MARGIN])):
        strip = jnp.concatenate(pair, axis=-1).transpose(2, 0, 1, 3, 4)
        strips.append(strip.reshape(b * m, LANES))
    return jnp.stack(slots), jnp.stack(side_slots), strips[0], strips[1]


def unpack_plain(plan, arrived):
    m, s, b = plan.members, plan.states, plan.bands
    bands = []
    for band in range(b):
        g, q = band // plan.patches, band % plan.patches
        pieces = jnp.stack(
            [arrived[plan.index_of[(g, c)], q * s : (q + 1) * s] for c in range(plan.patches)]
        )
        pieces = pieces.reshape(plan.patches, s, m, DEPTH, SPAN).transpose(2, 1, 3, 0, 4)
        bands.append(pieces.reshape(m, s, DEPTH, plan.cols))
    return jnp.concatenate(bands, axis=2)


def local(x, tally, cells, classes, readings, inverse, factors):
    count = lax.axis_size("mem")
    plan = Plan(x.shape, count, x.shape[1])
    patches = plan.patches
    index = lax.axis_index("mem")
    where = index.reshape(1)
    aligned = plan.members % (2 * HALF) == 0 and plan.rows % (2 * HALF) == 0
    states, members, total = plan.states, plan.members, plan.total
    strip = (plan.bands * members, LANES)
    side_slot = (count, plan.slot_bands + plan.map_groups, members, LANES)
    center_groups = plan.slot_bands * states
    if aligned:
        wide = DEPTH * plan.cols
        tables = (
            jax.ShapeDtypeStruct((HALF * HALF, HALF * HALF), bf16),
            jax.ShapeDtypeStruct((wide, wide), bf16),
        )
        turning, closing = pl.pallas_call(
            functools.partial(tables_kernel, plan),
            out_shape=tables,
            out_specs=(VMEM, VMEM),
            compiler_params=PARAMS,
            name="tables",
        )()
        packed, turned = pl.pallas_call(
            functools.partial(pack_kernel, plan),
            out_shape=(
                jax.ShapeDtypeStruct((count, center_groups, members, LANES), bf16),
                jax.ShapeDtypeStruct((states, plan.rows, members, plan.cols), bf16),
            ),
            in_specs=[VMEM, VMEM, VMEM],
            out_specs=(VMEM, VMEM),
            compiler_params=PARAMS,
            name="pack",
        )(x, turning, closing)
    else:
        packed, side_slots, upward, downward = pack_plain(plan, x)
    centers = lax.all_to_all(packed, "mem", split_axis=0, concat_axis=0, tiled=True)
    if aligned:
        own, upward, downward = pl.pallas_call(
            functools.partial(sides_kernel, plan),
            out_shape=(
                jax.ShapeDtypeStruct((patches,) + strip, bf16),
                jax.ShapeDtypeStruct(strip, bf16),
                jax.ShapeDtypeStruct(strip, bf16),
            ),
            in_specs=[VMEM],
            out_specs=(VMEM,) * 3,
            scratch_shapes=[
                pltpu.VMEM((states * DEPTH * plan.cols, (patches + 2) * LANES), bf16),
            ],
            compiler_params=PARAMS,
            name="sides",
        )(turned)
    forward, backward = shifts("col")
    left = lax.ppermute(upward, "col", forward)
    right = lax.ppermute(downward, "col", backward)
    slots = cells.shape[-1]
    maps = pl.pallas_call(
        functools.partial(map_kernel, patches, factors.shape[0]),
        out_shape=jax.ShapeDtypeStruct((patches, 4 * MAP_ROWS, LANES), bf16),
        in_specs=[SMEM, SMEM, VMEM, VMEM, VMEM, VMEM],
        out_specs=VMEM,
        compiler_params=PARAMS,
        name="maps",
    )(
        tally,
        factors,
        cells.reshape(patches, slots),
        classes.reshape(patches, slots),
        readings.reshape(patches, slots),
        inverse.reshape(patches, slots),
    )
    if aligned:
        parts = pl.pallas_call(
            functools.partial(join_kernel, plan),
            out_shape=(jax.ShapeDtypeStruct(side_slot[1:], bf16),) * count,
            in_specs=[SMEM, VMEM, VMEM, VMEM, VMEM],
            out_specs=(VMEM,) * count,
            scratch_shapes=[pltpu.VMEM(side_slot, bf16)],
            compiler_params=PARAMS,
            name="join",
        )(where, own, maps, left, right)
        arrived = [parts[0]] + [
            lax.ppermute(parts[k], "mem", [(i, i ^ k) for i in range(count)]) for k in range(1, count)
        ]
    else:
        for b in range(plan.bands):
            at = slice(b * members, (b + 1) * members)
            for column, extra in ((0, left[at]), (patches - 1, right[at])):
                for g, position in plan.band_slots(b):
                    side_slots = side_slots.at[plan.index_of[(g, column)], position].add(extra)
        for i, (g, c) in enumerate(plan.place):
            piece = jnp.where(index // patches == g, maps[c], 0).reshape(-1, members, LANES)
            side_slots = side_slots.at[i, plan.slot_bands :].set(piece)
        arrived = lax.all_to_all(side_slots, "mem", split_axis=0, concat_axis=0, tiled=True)
        centers, sides = (
            a.transpose(1, 0, 2, 3).reshape(1, -1, total, LANES)
            for a in (centers, arrived[:, : plan.slot_bands])
        )
        arrived = [sides, arrived[:, plan.slot_bands :].reshape(count, 1, 4 * MAP_ROWS, LANES)]
    pieces = (count, members) if aligned else (1, total)
    bands = patches + 2
    center_xs, center_avgs, *opening = pl.pallas_call(
        functools.partial(center_kernel, plan),
        out_shape=(
            jax.ShapeDtypeStruct((total, bands * states * LANES), bf16),
            jax.ShapeDtypeStruct((bands * 8, LANES), f32),
        )
        + (tables if aligned else ()),
        in_specs=[SMEM, VMEM],
        out_specs=(VMEM,) * (4 if aligned else 2),
        compiler_params=PARAMS,
        name="center",
    )(where, centers)
    depth = 3 * (states + 1) * LANES
    analysed = pl.pallas_call(
        functools.partial(analyse_kernel, plan, aligned),
        out_shape=jax.ShapeDtypeStruct((pieces[0], patches * states, pieces[1], LANES), bf16),
        in_specs=[SMEM, VMEM, VMEM] + [VMEM] * len(arrived),
        out_specs=VMEM,
        scratch_shapes=[
            pltpu.VMEM((total, bands * LANES), bf16),
            pltpu.VMEM((8, LANES), f32),
            pltpu.VMEM((patches, total + 16, depth), bf16),
            pltpu.VMEM((16, depth), f32),
            pltpu.VMEM(side_slot if aligned else (8, LANES), bf16),
        ],
        compiler_params=PARAMS,
        name="analyse",
    )(where, center_xs, center_avgs, *arrived)
    if not aligned:
        analysed = analysed.reshape(-1, count, plan.members, LANES).transpose(1, 0, 2, 3)
    returned = lax.all_to_all(analysed, "mem", split_axis=0, concat_axis=0, tiled=True)
    if not aligned:
        return unpack_plain(plan, returned)
    return pl.pallas_call(
        functools.partial(unpack_kernel, plan),
        out_shape=jax.ShapeDtypeStruct(x.shape, bf16),
        in_specs=[VMEM, VMEM, VMEM],
        out_specs=VMEM,
        scratch_shapes=[pltpu.VMEM((states, plan.rows, members, plan.cols), bf16)],
        compiler_params=PARAMS,
        name="unpack",
    )(returned, *opening)


def solution(mesh):
    placed = (
        P("mem", None, None, "col"),
        P("mem", "col"),
        P("mem", "col", None),
        P("mem", "col", None),
        P("mem", "col", None),
        P("mem", "col", None),
        P(),
    )
    return jax.shard_map(
        local, mesh=mesh, in_specs=placed, out_specs=P("mem", None, None, "col"), check_vma=False
    )
```

```python
import functools
import jax
import jax.numpy as jnp
from jax import lax
from jax.experimental import pallas as pl
from jax.experimental.pallas import tpu as pltpu
from jax.sharding import PartitionSpec as P

DEPTH = 4
SPAN = 32
MARGIN = 4
ITERS = 4
LANES = 128
HALF = 16
MAP_ROWS = 16
INFLATION = 1.1

f32 = jnp.float32
bf16 = jnp.bfloat16
i32 = jnp.int32
VMEM = pl.BlockSpec(memory_space=pltpu.VMEM)
SMEM = pl.BlockSpec(memory_space=pltpu.SMEM)
PARAMS = pltpu.CompilerParams(vmem_limit_bytes=14 * 1024 * 1024)


def iota(shape, dim):
    return lax.broadcasted_iota(i32, shape, dim)


def dot(a, b):
    return jnp.dot(a, b, preferred_element_type=f32)


def one_hot(condition):
    return jnp.where(condition, 1.0, 0.0).astype(bf16)


class Plan:
    def __init__(self, x_shape, count):
        self.members, self.states, self.rows, self.cols = x_shape
        self.count = count
        self.total = self.members * count
        self.patches = self.cols // SPAN
        self.bands = self.rows // DEPTH
        self.groups = self.bands // self.patches
        chips = count // 2
        if count % 2 == 0 and chips % self.patches == 0:
            self.place = [
                (2 * (i // 2 // self.patches) + i % 2, i // 2 % self.patches) for i in range(count)
            ]
        else:
            self.place = [(i // self.patches, i % self.patches) for i in range(count)]
        self.slot_bands = self.patches + min(2, self.groups - 1) if self.groups > 1 else self.patches
        self.full = self.slot_bands == self.patches + 2
        self.map_groups = 4 * MAP_ROWS // self.members
        self.index_of = {p: i for i, p in enumerate(self.place)}
        self.aligned = self.members % (2 * HALF) == 0 and self.rows % (2 * HALF) == 0
        self.aligned = self.aligned and count > 1 and count & (count - 1) == 0
        self.pair = self.aligned and self.groups == 2
        self.center_bands = self.patches if self.pair else self.slot_bands

    def group_of(self, index):
        return sum(jnp.where(index == i, g, 0) for i, (g, _) in enumerate(self.place))

    def shift_of(self, group):
        return jnp.where(group == 0, 0 if self.full else 1, 0)

    def first_band(self, group):
        low = self.patches * group - 1
        return low if self.full else max(low, 0)

    def band_slots(self, band):
        return [
            (g, band - self.first_band(g))
            for g in range(self.groups)
            if 0 <= band - self.first_band(g) < self.slot_bands
        ]

    def center_slots(self, band):
        if self.pair:
            return [(band // self.patches, band % self.patches)]
        return self.band_slots(band)


def side_source(lane, column):
    eighth = lane % (2 * MARGIN)
    low = column * SPAN - MARGIN + eighth
    high = column * SPAN + SPAN + eighth - MARGIN
    return jnp.where(eighth < MARGIN, low, high)


def turn_table():
    r = iota((HALF * HALF, HALF * HALF), 0)
    k = iota((HALF * HALF, HALF * HALF), 1)
    return one_hot((r % HALF == k // HALF) & (r // HALF == k % HALF))


def lane_table(cols, closing):
    wide = DEPTH * cols
    r = iota((wide, wide), 0 if closing else 1)
    k = iota((wide, wide), 1 if closing else 0)
    return one_hot(
        (r // cols == (k % LANES) // SPAN) & (r % cols == (k // LANES) * SPAN + k % SPAN)
    )


def turn(table, read, write, first, second):
    for a in range(0, first, HALF):
        for b in range(0, second, 2 * HALF):
            pair = [read(a, b + n * HALF).reshape(HALF * HALF, LANES) for n in range(2)]
            done = dot(table, jnp.concatenate(pair, axis=1)).astype(bf16)
            for n in range(2):
                piece = done[:, n * LANES : (n + 1) * LANES]
                write(a, b + n * HALF, piece.reshape(HALF, HALF, LANES))


def tables_kernel(plan, turn_ref, close_ref):
    turn_ref[...] = turn_table()
    close_ref[...] = lane_table(plan.cols, True)


def pack_kernel(plan, x_ref, turn_ref, close_ref, buf_ref, turned):
    table = turn_ref[...]
    m = plan.members
    for s in range(plan.states):
        def read(a, b):
            return x_ref[a : a + HALF, s, b : b + HALF]

        def write(a, b, piece):
            turned[s, b : b + HALF, a : a + HALF] = piece

        turn(table, read, write, m, plan.rows)
        center = dot(banded(plan, turned, s), close_ref[...]).astype(bf16)
        for b in range(plan.bands):
            for c in range(plan.patches):
                value = center[b * m : (b + 1) * m, c * LANES : (c + 1) * LANES]
                for g, position in plan.center_slots(b):
                    buf_ref[plan.index_of[(g, c)], position * plan.states + s] = value
    if plan.full:
        zero = jnp.zeros((plan.members, LANES), bf16)
        for c in range(plan.patches):
            for s in range(plan.states):
                buf_ref[plan.index_of[(0, c)], s] = zero
                last = (plan.slot_bands - 1) * plan.states + s
                buf_ref[plan.index_of[(plan.groups - 1, c)], last] = zero


def banded(plan, turned, s):
    return jnp.concatenate(
        [
            jnp.concatenate([turned[s, b * DEPTH + t] for b in range(plan.bands)], axis=0)
            for t in range(DEPTH)
        ],
        axis=1,
    )


def sides_kernel(plan, turned, own_ref, up_ref, down_ref, side_ref):
    cols = plan.cols
    n_side = (plan.patches + 2) * LANES
    col = iota((cols, n_side), 0)
    out = iota((cols, n_side), 1)
    column = out // LANES
    lane = out % LANES
    eighth = lane % (2 * MARGIN)
    source = side_source(lane, column)
    to_up = (column == plan.patches) & (eighth < MARGIN)
    to_down = (column == plan.patches + 1) & (eighth >= MARGIN)
    source = jnp.where(column < plan.patches, source, -1)
    source = jnp.where(to_up, cols - MARGIN + eighth, source)
    source = jnp.where(to_down, eighth - MARGIN, source)
    hit = jnp.where(col == source, 1.0, 0.0)
    which = iota((1, n_side), 1) % LANES // (2 * MARGIN)
    for s in range(plan.states):
        for t in range(DEPTH):
            at = s * DEPTH + t
            side_ref[at * cols : (at + 1) * cols, :] = jnp.where(which == at, hit, 0.0).astype(bf16)
    lhs = jnp.concatenate([banded(plan, turned, s) for s in range(plan.states)], axis=1)
    sides = dot(lhs, side_ref[...]).astype(bf16)
    for c in range(plan.patches):
        own_ref[c] = sides[:, c * LANES : (c + 1) * LANES]
    at = plan.patches * LANES
    up_ref[...] = sides[:, at : at + LANES]
    down_ref[...] = sides[:, at + LANES : at + 2 * LANES]


def split2(a):
    high = a.astype(bf16)
    return high, (a - high.astype(f32)).astype(bf16)


def window_place(entry):
    height = DEPTH + 2 * MARGIN
    width = SPAN + 2 * MARGIN
    plane = height * width
    state = sum((entry >= plane * n).astype(i32) for n in range(1, 4))
    rest = entry - state * plane
    row = (rest * 1639) >> 16
    col = rest - row * width
    band = row >> 2
    inner = row & 3
    center = (col >= MARGIN) & (col < MARGIN + SPAN)
    eighth = jnp.where(col < MARGIN, col, col - SPAN)
    lane = jnp.where(center, inner * SPAN + col - MARGIN, state * SPAN + inner * 2 * MARGIN + eighth)
    group = jnp.where(center, band * 4 + state, 12 + band)
    return group, lane


def map_kernel(patches, table, count_ref, factor_ref, cell_ref, class_ref, value_ref, inv_ref, out_ref):
    slots = cell_ref.shape[1]
    group, lane = window_place(cell_ref[...])
    classes = class_ref[...]
    factor = jnp.zeros(classes.shape, f32)
    for n in range(table):
        factor = jnp.where(classes == n, factor_ref[n], factor)
    weight = inv_ref[...] * factor
    order = iota((1, slots), 1)
    for p in range(patches):
        live = jnp.where(order < count_ref[0, p], weight[p : p + 1], 0.0)
        hot = one_hot(iota((LANES, slots), 0) == lane[p : p + 1])
        pick = iota((MAP_ROWS, slots), 0) == group[p : p + 1]
        parts = []
        for source in (live, live * value_ref[p : p + 1]):
            for _ in range(3):
                high = source.astype(bf16).astype(f32)
                parts.append(jnp.where(pick, high, 0.0).astype(bf16))
                source = source - high
        maps = lax.dot_general(
            jnp.concatenate(parts, axis=0), hot, (((1,), (1,)), ((), ())), preferred_element_type=f32
        )
        n = MAP_ROWS
        w_high, w_low = split2(maps[:n] + maps[n : 2 * n] + maps[2 * n : 3 * n])
        v_high, v_low = split2(maps[3 * n : 4 * n] + maps[4 * n : 5 * n] + maps[5 * n :])
        out_ref[p] = jnp.concatenate([w_high, w_low, v_high, v_low], axis=0)


def join_kernel(plan, place_ref, own_ref, maps_ref, left_ref, right_ref, *outs):
    buf_ref = outs[-1]
    index = place_ref[0]
    m = plan.members
    zero = jnp.zeros((m, LANES), bf16)
    for b in range(plan.bands):
        at = slice(b * m, (b + 1) * m)
        for c in range(plan.patches):
            value = own_ref[c, at]
            if c == 0:
                value = value + left_ref[at]
            if c == plan.patches - 1:
                value = value + right_ref[at]
            for g, position in plan.band_slots(b):
                buf_ref[plan.index_of[(g, c)], position] = value
    if plan.full:
        for c in range(plan.patches):
            buf_ref[plan.index_of[(0, c)], 0] = zero
            buf_ref[plan.index_of[(plan.groups - 1, c)], plan.slot_bands - 1] = zero
    for i, (g, c) in enumerate(plan.place):
        piece = jnp.where(index // plan.patches == g, maps_ref[c], jnp.zeros_like(maps_ref[c]))
        for n in range(plan.map_groups):
            buf_ref[i, plan.slot_bands + n] = piece[n * m : (n + 1) * m]
    own_half, other_half, _ = outs
    for k in range(plan.count // 2):
        own_half[k] = buf_ref[index ^ (2 * k)]
        other_half[k] = buf_ref[index ^ (2 * k + 1)]


def merge_kernel(own_ref, other_ref, *outs):
    for k, out in enumerate(outs):
        out[0] = own_ref[k]
        out[1] = other_ref[k]


def mm2(a, b):
    return dot(jnp.concatenate(split2(a), axis=1), jnp.concatenate([b, b], axis=0))


def center_of(plan, shift, fields, count, width, xs, avgs):
    sources = fields.shape[0]
    total, patches = plan.total, plan.patches
    step = 8 if width > 1 else 1
    if count < patches + 2:
        edges = (0, patches + 1)
        if count > patches:
            edges = (jnp.where(shift == 1, 0, patches + 1),)
        for edge in edges:
            lanes = pl.ds(edge * width * LANES, width * LANES)
            if not isinstance(edge, int):
                lanes = pl.ds(pl.multiple_of(edge * width * LANES, LANES), width * LANES)
            xs[:, lanes] = jnp.zeros((total, width * LANES), bf16)
            avgs[pl.ds(edge * step, step)] = jnp.zeros((step, LANES), f32)
    for b in range(count):
        means = []
        for inner in range(width):
            at = b * width + inner
            raw = jnp.concatenate([fields[n, at] for n in range(sources)], axis=0).astype(f32)
            mean = jnp.sum(raw, axis=0, keepdims=True) / total
            means.append(mean)
            lanes = ((shift + b) * width + inner) * LANES
            if not isinstance(lanes, int):
                lanes = pl.multiple_of(lanes, LANES)
            xs[:, pl.ds(lanes, LANES)] = (raw - mean).astype(bf16)
        if width > 1:
            means.append(jnp.zeros((step - width, LANES), f32))
        avgs[pl.ds((b + shift) * step, step)] = jnp.concatenate(means, axis=0)


def center_kernel(plan, place_ref, x_ref, xs, avgs, turn_ref=None, open_ref=None, send_ref=None):
    if open_ref is not None:
        turn_ref[...] = turn_table()
        open_ref[...] = lane_table(plan.cols, False)
    if send_ref is not None:
        near = jnp.where(plan.group_of(place_ref[0]) == 0, plan.patches - 1, 0)
        for n in range(x_ref.shape[0]):
            for s in range(plan.states):
                send_ref[n, s] = x_ref[n, near * plan.states + s]
    shift = 1 if plan.pair else plan.shift_of(plan.group_of(place_ref[0]))
    center_of(plan, shift, x_ref, plan.center_bands, plan.states, xs, avgs)


def analyse_kernel(
    plan, relative, place_ref, xs, avgs, *rest
):
    *pieces, out_ref, side_xs, side_avgs, scaled, lead, gathered, edge_xs, edge_avgs = rest

    total, states, patches = plan.total, plan.states, plan.patches
    sources, _, piece_rows, _ = out_ref.shape
    group = plan.group_of(place_ref[0])
    if relative:
        for k in range(plan.count):
            gathered[place_ref[0] ^ k] = pieces[k // 2][k % 2]
    if plan.pair:
        near = pieces[-1]
        wide = states * LANES
        at = pl.multiple_of(jnp.where(group == 0, wide, 0), LANES)
        edge_xs[:, pl.ds(pl.multiple_of(wide - at, LANES), wide)] = jnp.zeros((total, wide), bf16)
        edge_avgs[...] = jnp.zeros_like(edge_avgs)
        means = []
        for s in range(states):
            raw = jnp.concatenate([near[n, s] for n in range(near.shape[0])], axis=0).astype(f32)
            means.append(jnp.sum(raw, axis=0, keepdims=True) / total)
            edge_xs[:, pl.ds(pl.multiple_of(at + s * LANES, LANES), LANES)] = (
                raw - means[-1]
            ).astype(bf16)
        means.append(jnp.zeros((8 - states, LANES), f32))
        edge_avgs[pl.ds(jnp.where(group == 0, 8, 0), 8)] = jnp.concatenate(means, axis=0)

    def block(band):
        if plan.pair and band in (0, patches + 1):
            end = int(band > 0)
            return edge_xs, end * states * LANES, edge_avgs, end * 8
        return xs, band * states * LANES, avgs, band * 8

    if relative:
        side_ref, maps_ref, map_at = gathered, gathered, plan.slot_bands
    else:
        (side_ref, maps_ref), map_at = pieces, 0
    center_of(plan, plan.shift_of(group), side_ref, plan.slot_bands, 1, side_xs, side_avgs)
    eye = jnp.where(iota((total, total), 0) == iota((total, total), 1), 1.0, 0.0)
    grams, forcings, norms = [], [], []
    for q in range(patches):
        n_map = maps_ref.shape[1] - map_at
        maps = jnp.concatenate(
            [maps_ref[patches * group + q, map_at + n] for n in range(n_map)], axis=0
        ).astype(f32)
        n = MAP_ROWS
        weight = maps[:n] + maps[n : 2 * n]
        value = maps[2 * n : 3 * n] + maps[3 * n :]
        lead[...] = jnp.zeros_like(lead)
        for at in range(3 * (states + 1)):
            if at < 3 * states:
                band_xs, lanes, band_avgs, row = block(q + at // states)
                lanes, row = lanes + at % states * LANES, row + at % states
                source = band_xs[:, lanes : lanes + LANES]
                mean = band_avgs[row : row + 1]
            else:
                row = q + at - 3 * states
                source = side_xs[:, row * LANES : (row + 1) * LANES]
                mean = side_avgs[row : row + 1]
            w = weight[at : at + 1]
            here = slice(at * LANES, (at + 1) * LANES)
            scaled[q, :total, here] = (source.astype(f32) * w).astype(bf16)
            v = value[at : at + 1] - w * mean
            for part in range(3):
                high = v.astype(bf16).astype(f32)
                lead[part : part + 1, here] = high
                v = v - high
        scaled[q, total:] = lead[...].astype(bf16)
        window = []
        for band in range(q, q + 3):
            band_xs, lanes, _, _ = block(band)
            window.append(band_xs[:, lanes : lanes + states * LANES])
        window.append(side_xs[:, q * LANES : (q + 3) * LANES])
        window = jnp.concatenate(window, axis=1)
        both = lax.dot_general(
            scaled[q], window, (((1,), (1,)), ((), ())), preferred_element_type=f32
        )
        gram = both[:total] + ((total - 1) / INFLATION) * eye
        forcings.append(both[total : total + 1] + both[total + 1 : total + 2] + both[total + 2 : total + 3])
        norm = jnp.sqrt(jnp.sum(jnp.sum(gram * gram, axis=1, keepdims=True), axis=0, keepdims=True))
        norms.append(norm)
        grams.append(gram / norm)
    scale = 1.5
    iterates, rests = [], []
    for q in range(patches):
        iterates.append(1.5 * grams[q] - 0.5 * mm2(grams[q], grams[q].astype(bf16)))
        rests.append(-0.5 * grams[q])
    for sweep in range(1, ITERS):
        last = sweep + 1 == ITERS
        for q in range(patches):
            y = iterates[q].astype(bf16)
            product = scale * iterates[q] + mm2(rests[q], y)
            rest = rests[q].astype(bf16)
            both = mm2(product, rest if last else jnp.concatenate([rest, y], axis=1))
            rests[q] = 1.5 * rests[q] - 0.5 * (scale * product + both[:, :total])
            if not last:
                iterates[q] = 1.5 * iterates[q] - 0.5 * both[:, total:]
        scale = scale * 1.5
    roots = [scale * eye + rest for rest in rests]
    for q in range(patches):
        root = roots[q]
        force = jnp.broadcast_to(forcings[q], (8, total))
        high, low = split2(root)
        tall = jnp.concatenate([high, high, low], axis=0)

        def apply(v):
            h, l = split2(v)
            return dot(jnp.concatenate([h, l, h], axis=1), tall)

        move = apply(apply(force))
        move = move[:1] / norms[q]
        transform = (jnp.sqrt((total - 1.0) / norms[q]) * root + move).astype(bf16)
        first = (q + 1) * states * LANES
        analysed = dot(transform, xs[:, first : first + states * LANES])
        for s in range(states):
            row = (q + 1) * 8 + s
            value = (analysed[:, s * LANES : (s + 1) * LANES] + avgs[row : row + 1]).astype(bf16)
            for n in range(sources):
                out_ref[n, q * states + s] = value[n * piece_rows : (n + 1) * piece_rows]


def unpack_kernel(plan, in_ref, turn_ref, open_ref, out_ref, turned):
    m, rows, cols, states = plan.members, plan.rows, plan.cols, plan.states
    table = turn_ref[...]
    for s in range(states):
        lhs = []
        for b in range(plan.bands):
            g, q = b // plan.patches, b % plan.patches
            lhs.append(
                jnp.concatenate(
                    [in_ref[plan.index_of[(g, c)], q * states + s] for c in range(plan.patches)], axis=1
                )
            )
        opened = dot(jnp.concatenate(lhs, axis=0), open_ref[...]).astype(bf16)
        for b in range(plan.bands):
            for t in range(DEPTH):
                turned[s, b * DEPTH + t] = opened[b * m : (b + 1) * m, t * cols : (t + 1) * cols]

        def read(a, b):
            return turned[s, a : a + HALF, b : b + HALF]

        def write(a, b, piece):
            out_ref[b : b + HALF, s, a : a + HALF] = piece

        turn(table, read, write, rows, m)


def shifts(axis):
    count = lax.axis_size(axis)
    forward = [(i, i + 1) for i in range(count - 1)]
    return forward, [(b, a) for a, b in forward]


def pack_plain(plan, x):
    m, s, b = plan.members, plan.states, plan.bands
    bands = x.reshape(m, s, b, DEPTH, plan.cols)
    center = bands.reshape(m, s, b, DEPTH, plan.patches, SPAN).transpose(4, 2, 1, 0, 3, 5)
    center = center.reshape(plan.patches, b, s, m, LANES)
    padded = jnp.pad(bands, ((0, 0),) * 4 + ((MARGIN, MARGIN),))
    sides = jnp.stack(
        [
            jnp.concatenate(
                [
                    padded[..., c * SPAN : c * SPAN + MARGIN],
                    padded[..., (c + 1) * SPAN + MARGIN : (c + 1) * SPAN + 2 * MARGIN],
                ],
                axis=-1,
            )
            for c in range(plan.patches)
        ]
    )
    sides = sides.transpose(0, 3, 1, 2, 4, 5).reshape(plan.patches, b, 1, m, LANES)
    center, sides = (jnp.pad(a, ((0, 0), (1, 1)) + ((0, 0),) * 3) for a in (center, sides))
    slots, side_slots = [], []
    for g, c in plan.place:
        at = slice(plan.first_band(g) + 1, plan.first_band(g) + 1 + plan.slot_bands)
        slots.append(center[c, at].reshape(-1, m, LANES))
        side_slots.append(jnp.pad(sides[c, at, 0], ((0, plan.map_groups), (0, 0), (0, 0))))
    empty = jnp.zeros_like(bands[..., :MARGIN])
    strips = []
    for pair in ((bands[..., -MARGIN:], empty), (empty, bands[..., :MARGIN])):
        strip = jnp.concatenate(pair, axis=-1).transpose(2, 0, 1, 3, 4)
        strips.append(strip.reshape(b * m, LANES))
    return jnp.stack(slots), jnp.stack(side_slots), strips[0], strips[1]


def unpack_plain(plan, arrived):
    m, s, b = plan.members, plan.states, plan.bands
    bands = []
    for band in range(b):
        g, q = band // plan.patches, band % plan.patches
        pieces = jnp.stack(
            [arrived[plan.index_of[(g, c)], q * s : (q + 1) * s] for c in range(plan.patches)]
        )
        pieces = pieces.reshape(plan.patches, s, m, DEPTH, SPAN).transpose(2, 1, 3, 0, 4)
        bands.append(pieces.reshape(m, s, DEPTH, plan.cols))
    return jnp.concatenate(bands, axis=2)


def local(x, tally, cells, classes, readings, inverse, factors):
    count = lax.axis_size("mem")
    plan = Plan(x.shape, count)
    patches = plan.patches
    index = lax.axis_index("mem")
    where = index.reshape(1)
    aligned = plan.aligned
    states, members, total = plan.states, plan.members, plan.total
    strip = (plan.bands * members, LANES)
    side_slot = (count, plan.slot_bands + plan.map_groups, members, LANES)
    center_groups = plan.center_bands * states
    if aligned:
        wide = DEPTH * plan.cols
        tables = (
            jax.ShapeDtypeStruct((HALF * HALF, HALF * HALF), bf16),
            jax.ShapeDtypeStruct((wide, wide), bf16),
        )
        turning, closing = pl.pallas_call(
            functools.partial(tables_kernel, plan),
            out_shape=tables,
            out_specs=(VMEM, VMEM),
            compiler_params=PARAMS,
            name="tables",
        )()
        packed, turned = pl.pallas_call(
            functools.partial(pack_kernel, plan),
            out_shape=(
                jax.ShapeDtypeStruct((count, center_groups, members, LANES), bf16),
                jax.ShapeDtypeStruct((states, plan.rows, members, plan.cols), bf16),
            ),
            in_specs=[VMEM, VMEM, VMEM],
            out_specs=(VMEM, VMEM),
            compiler_params=PARAMS,
            name="pack",
        )(x, turning, closing)
    else:
        packed, side_slots, upward, downward = pack_plain(plan, x)
    centers = lax.all_to_all(packed, "mem", split_axis=0, concat_axis=0, tiled=True)
    if aligned:
        own, upward, downward = pl.pallas_call(
            functools.partial(sides_kernel, plan),
            out_shape=(
                jax.ShapeDtypeStruct((patches,) + strip, bf16),
                jax.ShapeDtypeStruct(strip, bf16),
                jax.ShapeDtypeStruct(strip, bf16),
            ),
            in_specs=[VMEM],
            out_specs=(VMEM,) * 3,
            scratch_shapes=[
                pltpu.VMEM((states * DEPTH * plan.cols, (patches + 2) * LANES), bf16),
            ],
            compiler_params=PARAMS,
            name="sides",
        )(turned)
    forward, backward = shifts("col")
    left = lax.ppermute(upward, "col", forward)
    right = lax.ppermute(downward, "col", backward)
    slots = cells.shape[-1]
    maps = pl.pallas_call(
        functools.partial(map_kernel, patches, factors.shape[0]),
        out_shape=jax.ShapeDtypeStruct((patches, 4 * MAP_ROWS, LANES), bf16),
        in_specs=[SMEM, SMEM, VMEM, VMEM, VMEM, VMEM],
        out_specs=VMEM,
        compiler_params=PARAMS,
        name="maps",
    )(
        tally,
        factors,
        cells.reshape(patches, slots),
        classes.reshape(patches, slots),
        readings.reshape(patches, slots),
        inverse.reshape(patches, slots),
    )
    if aligned:
        pairs = count // 2
        half = jax.ShapeDtypeStruct((pairs,) + side_slot[1:], bf16)
        own_half, other_half = pl.pallas_call(
            functools.partial(join_kernel, plan),
            out_shape=(half, half),
            in_specs=[SMEM, VMEM, VMEM, VMEM, VMEM],
            out_specs=(VMEM, VMEM),
            scratch_shapes=[pltpu.VMEM(side_slot, bf16)],
            compiler_params=PARAMS,
            name="join",
        )(where, own, maps, left, right)
        other_half = lax.ppermute(other_half, "mem", [(i, i ^ 1) for i in range(count)])
        parts = pl.pallas_call(
            merge_kernel,
            out_shape=(jax.ShapeDtypeStruct((2,) + side_slot[1:], bf16),) * pairs,
            in_specs=[VMEM, VMEM],
            out_specs=(VMEM,) * pairs,
            compiler_params=PARAMS,
            name="merge",
        )(own_half, other_half)
        arrived = [parts[0]]
        for k in range(1, pairs):
            pairing = [(i, i ^ (2 * k)) for i in range(count)]
            arrived.append(lax.ppermute(parts[k], "mem", pairing))
    else:
        for b in range(plan.bands):
            at = slice(b * members, (b + 1) * members)
            for column, extra in ((0, left[at]), (patches - 1, right[at])):
                for g, position in plan.band_slots(b):
                    side_slots = side_slots.at[plan.index_of[(g, column)], position].add(extra)
        for i, (g, c) in enumerate(plan.place):
            piece = jnp.where(index // patches == g, maps[c], 0).reshape(-1, members, LANES)
            side_slots = side_slots.at[i, plan.slot_bands :].set(piece)
        arrived = lax.all_to_all(side_slots, "mem", split_axis=0, concat_axis=0, tiled=True)
        centers, sides = (
            a.transpose(1, 0, 2, 3).reshape(1, -1, total, LANES)
            for a in (centers, arrived[:, : plan.slot_bands])
        )
        arrived = [sides, arrived[:, plan.slot_bands :].reshape(count, 1, 4 * MAP_ROWS, LANES)]
    pieces = (count, members) if aligned else (1, total)
    bands = patches + 2
    center_xs, center_avgs, *opening = pl.pallas_call(
        functools.partial(center_kernel, plan),
        out_shape=(
            jax.ShapeDtypeStruct((total, bands * states * LANES), bf16),
            jax.ShapeDtypeStruct((bands * 8, LANES), f32),
        )
        + (tables if aligned else ())
        + ((jax.ShapeDtypeStruct((count, states, members, LANES), bf16),) if plan.pair else ()),
        in_specs=[SMEM, VMEM],
        out_specs=(VMEM,) * (2 + 2 * aligned + plan.pair),
        compiler_params=PARAMS,
        name="center",
    )(where, centers)
    if plan.pair:
        other = [(i, plan.index_of[(1 - g, c)]) for i, (g, c) in enumerate(plan.place)]
        arrived.append(lax.ppermute(opening.pop(), "mem", other))
    depth = 3 * (states + 1) * LANES
    analysed = pl.pallas_call(
        functools.partial(analyse_kernel, plan, aligned),
        out_shape=jax.ShapeDtypeStruct((pieces[0], patches * states, pieces[1], LANES), bf16),
        in_specs=[SMEM, VMEM, VMEM] + [VMEM] * len(arrived),
        out_specs=VMEM,
        scratch_shapes=[
            pltpu.VMEM((total, bands * LANES), bf16),
            pltpu.VMEM((8, LANES), f32),
            pltpu.VMEM((patches, total + 16, depth), bf16),
            pltpu.VMEM((16, depth), f32),
            pltpu.VMEM(side_slot if aligned else (8, LANES), bf16),
            pltpu.VMEM((total, 2 * states * LANES), bf16),
            pltpu.VMEM((16, LANES), f32),
        ],
        compiler_params=PARAMS,
        name="analyse",
    )(where, center_xs, center_avgs, *arrived)
    if not aligned:
        analysed = analysed.reshape(-1, count, plan.members, LANES).transpose(1, 0, 2, 3)
    returned = lax.all_to_all(analysed, "mem", split_axis=0, concat_axis=0, tiled=True)
    if not aligned:
        return unpack_plain(plan, returned)
    return pl.pallas_call(
        functools.partial(unpack_kernel, plan),
        out_shape=jax.ShapeDtypeStruct(x.shape, bf16),
        in_specs=[VMEM, VMEM, VMEM],
        out_specs=VMEM,
        scratch_shapes=[pltpu.VMEM((states, plan.rows, members, plan.cols), bf16)],
        compiler_params=PARAMS,
        name="unpack",
    )(returned, *opening)


def solution(mesh):
    placed = (
        P("mem", None, None, "col"),
        P("mem", "col"),
        P("mem", "col", None),
        P("mem", "col", None),
        P("mem", "col", None),
        P("mem", "col", None),
        P(),
    )

    return jax.shard_map(
        local, mesh=mesh, in_specs=placed, out_specs=P("mem", None, None, "col"), check_vma=False
    )
```
